128 devices in a mesh: data: 128 (over z, y, x, core).
Axes of the slice: x: 4, y: 4, z: 4, core: 2. Of those that a mesh axis runs over, the one named last changes fastest.
Arguments:
- q_in: bfloat16 [8192, 512], P('data')
- d_in: bfloat16 [2, 8192, 512], P(None, 'data')
- temperature: float32 [], replicated
- q_w1: bfloat16 [2, 512, 2048], replicated
- q_w2: bfloat16 [2, 2048, 512], replicated
- q_proj: bfloat16 [512, 512], replicated
- d_w1: bfloat16 [2, 512, 2048], replicated
- d_w2: bfloat16 [2, 2048, 512], replicated
- d_proj: bfloat16 [512, 512], replicated
Outputs:
- output 1: float32 [], replicated
- output 2: float32 [2, 512, 2048], replicated
- output 3: float32 [2, 2048, 512], replicated
- output 4: float32 [512, 512], replicated
- output 5: float32 [2, 512, 2048], replicated
- output 6: float32 [2, 2048, 512], replicated
- output 7: float32 [512, 512], replicated
All inputs are finite; a program needn't handle non-finite values.
Results may differ from the reference program's by a relative error of at most 0.00628917.
Values are sent between devices in bfloat16 or wider.
A program may use at most 1 GiB of HBM per device.

```python
import math
import jax
import jax.numpy as jnp
from jax import lax

GLOBAL_BATCH = 8192
SHARD_ROWS = 64
HIDDEN = 512
FFN_WIDTH = 2048
REPR_DIM = 512


def setup_inputs(seed: int = 0) -> dict:
    key_list = jax.random.split(jax.random.key(seed), 9)
    sharpness = 0.8 * math.sqrt(2.0 * math.log(2.0 * GLOBAL_BATCH))
    tau_base = 2.0 * math.sqrt(REPR_DIM) / sharpness

    def weight(w_key, w_shape, fan_in):
        return (jax.random.normal(w_key, w_shape, jnp.float32) * fan_in ** -0.5).astype(jnp.bfloat16)

    return dict(
        q_in=jax.random.normal(key_list[0], (GLOBAL_BATCH, HIDDEN), jnp.float32).astype(jnp.bfloat16),
        d_in=jax.random.normal(key_list[1], (2, GLOBAL_BATCH, HIDDEN), jnp.float32).astype(jnp.bfloat16),
        temperature=tau_base * jax.random.uniform(key_list[2], (), jnp.float32, 0.8, 1.25),
        q_w1=weight(key_list[3], (2, HIDDEN, FFN_WIDTH), HIDDEN),
        q_w2=weight(key_list[4], (2, FFN_WIDTH, HIDDEN), FFN_WIDTH),
        q_proj=weight(key_list[5], (HIDDEN, REPR_DIM), HIDDEN),
        d_w1=weight(key_list[6], (2, HIDDEN, FFN_WIDTH), HIDDEN),
        d_w2=weight(key_list[7], (2, FFN_WIDTH, HIDDEN), FFN_WIDTH),
        d_proj=weight(key_list[8], (HIDDEN, REPR_DIM), HIDDEN),
    )


def tower_forward(row_block, w_one, w_two, w_proj):
    hidden = row_block
    saved = []
    for layer in range(2):
        pre_act = jnp.dot(hidden, w_one[layer], preferred_element_type=jnp.float32)
        act_bf = jax.nn.gelu(pre_act).astype(jnp.bfloat16)
        saved.append((hidden, pre_act, act_bf))
        hidden = (hidden.astype(jnp.float32) + jnp.dot(act_bf, w_two[layer], preferred_element_type=jnp.float32)).astype(jnp.bfloat16)
    out_reps = jnp.dot(hidden, w_proj, preferred_element_type=jnp.float32).astype(jnp.bfloat16)
    return out_reps, hidden, saved


def tower_backward(upstream, w_one, w_two, w_proj, hidden, saved):
    g_proj = jnp.dot(hidden.T, upstream, preferred_element_type=jnp.float32)
    resid_grad = jnp.dot(upstream, w_proj.T, preferred_element_type=jnp.float32)
    grads_one = [None, None]
    grads_two = [None, None]
    for layer in (1, 0):
        h_in, pre_act, act_bf = saved[layer]
        resid_bf = resid_grad.astype(jnp.bfloat16)
        grads_two[layer] = jnp.dot(act_bf.T, resid_bf, preferred_element_type=jnp.float32)
        act_grad = jnp.dot(resid_bf, w_two[layer].T, preferred_element_type=jnp.float32)
        gelu_back = jax.vjp(jax.nn.gelu, pre_act)[1]
        pre_grad = gelu_back(act_grad)[0].astype(jnp.bfloat16)
        grads_one[layer] = jnp.dot(h_in.T, pre_grad, preferred_element_type=jnp.float32)
        if layer == 1:
            resid_grad = resid_grad + jnp.dot(pre_grad, w_one[layer].T, preferred_element_type=jnp.float32)
    return jnp.stack(grads_one), jnp.stack(grads_two), g_proj


def tower_grads(row_blocks, up_blocks, w_one, w_two, w_proj):
    def body(running, block_in):
        row_block, upstream = block_in
        hidden, saved = tower_forward(row_block, w_one, w_two, w_proj)[1:]
        new_grads = tower_backward(upstream, w_one, w_two, w_proj, hidden, saved)
        return tuple(old_sum + new_part for old_sum, new_part in zip(running, new_grads)), None

    zeros_init = (jnp.zeros(w_one.shape, jnp.float32), jnp.zeros(w_two.shape, jnp.float32), jnp.zeros(w_proj.shape, jnp.float32))
    return lax.scan(body, zeros_init, (row_blocks, up_blocks))[0]


def reference(q_in, d_in, temperature, q_w1, q_w2, q_proj, d_w1, d_w2, d_proj):
    n_blocks = GLOBAL_BATCH // SHARD_ROWS
    q_blocks = q_in.reshape(n_blocks, SHARD_ROWS, HIDDEN)
    d_blocks = d_in.reshape(n_blocks, 2 * SHARD_ROWS, HIDDEN)
    q_reps = lax.map(lambda row_block: tower_forward(row_block, q_w1, q_w2, q_proj)[0], q_blocks)
    doc_flat = lax.map(lambda row_block: tower_forward(row_block, d_w1, d_w2, d_proj)[0], d_blocks).reshape(2 * GLOBAL_BATCH, REPR_DIM)
    col_index = jnp.arange(2 * GLOBAL_BATCH)

    def loss_block(running, block_in):
        loss_sum, doc_grad = running
        q_block, block_index = block_in
        logits = jnp.dot(q_block, doc_flat.T, preferred_element_type=jnp.float32) / temperature
        row_index = block_index * SHARD_ROWS + jnp.arange(SHARD_ROWS)
        target = col_index[None, :] == row_index[:, None]
        log_norm = jax.nn.logsumexp(logits, axis=1)
        pos_logit = jnp.sum(jnp.where(target, logits, 0.0), axis=1)
        soft_prob = jnp.exp(logits - log_norm[:, None])
        grad_logit = ((soft_prob - target.astype(jnp.float32)) / (GLOBAL_BATCH * temperature)).astype(jnp.bfloat16)
        q_up = jnp.dot(grad_logit, doc_flat, preferred_element_type=jnp.float32).astype(jnp.bfloat16)
        doc_grad = doc_grad + jnp.dot(grad_logit.T, q_block, preferred_element_type=jnp.float32)
        return (loss_sum + jnp.sum(log_norm - pos_logit), doc_grad), q_up

    zeros_init = (jnp.zeros((), jnp.float32), jnp.zeros((2 * GLOBAL_BATCH, REPR_DIM), jnp.float32))
    final_state, q_up_blocks = lax.scan(loss_block, zeros_init, (q_reps, jnp.arange(n_blocks)))
    loss_sum, doc_grad = final_state
    doc_up_blocks = doc_grad.astype(jnp.bfloat16).reshape(n_blocks, 2 * SHARD_ROWS, REPR_DIM)
    q_one, q_two, q_pgrad = tower_grads(q_blocks, q_up_blocks, q_w1, q_w2, q_proj)
    d_one, d_two, d_pgrad = tower_grads(d_blocks, doc_up_blocks, d_w1, d_w2, d_proj)
    return (loss_sum / GLOBAL_BATCH, q_one, q_two, q_pgrad, d_one, d_two, d_pgrad)
```

```python
import functools

import jax
import jax.numpy as jnp
from jax import lax
from jax.experimental import pallas as pl
from jax.experimental.pallas import tpu as pltpu
from jax.sharding import PartitionSpec as P

F32 = jnp.float32
BF16 = jnp.bfloat16
MESH = pl.DeviceIdType.MESH
SUB_COUNT = 4
SIDE = 4
ROWS_CONTRACT = (((0,), (0,)), ((), ()))
LAST_CONTRACT = (((1,), (1,)), ((), ()))
VMEM_LIMIT = 67043328

UNITS = 1088
COLOUR_OFFSET = (0, 384, 768)
COLOUR_ROWS = (6, 6, 5)
COLOUR_DIMS = (('x', 'y', 'z'), ('y', 'z', 'x'), ('z', 'x', 'y'))


def place():
    me = lax.axis_index('data')
    core = lax.rem(me, 2)
    x = lax.rem(me // 2, SIDE)
    y = lax.rem(me // 8, SIDE)
    z = me // 32
    return dict(z=z, y=y, x=x, core=core)


def device(at):
    return (((at['z'] * SIDE + at['y']) * SIDE + at['x']) * 2 + at['core'],)


def moved(at, dim, step):
    size = 2 if dim == 'core' else SIDE
    return {**at, dim: lax.rem(at[dim] + step, size)}


def dot(lhs, rhs, dims=None):
    if dims is None:
        return jnp.dot(lhs, rhs, preferred_element_type=F32)
    return lax.dot_general(lhs, rhs, dims, preferred_element_type=F32)


def tower_forward(rows, w_one, w_two, w_proj):
    hidden = rows
    for layer in range(2):
        act = jax.nn.gelu(dot(hidden, w_one[layer])).astype(BF16)
        hidden = (hidden.astype(F32) + dot(act, w_two[layer])).astype(BF16)
    return dot(hidden, w_proj[...]).astype(BF16)


def forward_kernel(q_in, d_in, q_w1, q_w2, q_proj, d_w1, d_w2, d_proj, q_out, d_out):
    def body(sub, carry):
        rows = pl.ds(pl.multiple_of(sub * 16, 16), 16)
        q_out[rows, :] = tower_forward(q_in[rows, :], q_w1, q_w2, q_proj)
        rows = pl.ds(pl.multiple_of(sub * 32, 32), 32)
        d_out[rows, :] = tower_forward(d_in[rows, :], d_w1, d_w2, d_proj)
        return carry

    lax.fori_loop(0, SUB_COUNT, body, 0)


def forward(q_rows, d_rows, weights):
    vmem = pl.BlockSpec(memory_space=pltpu.VMEM)
    return pl.pallas_call(
        forward_kernel,
        out_shape=(jax.ShapeDtypeStruct(q_rows.shape, BF16), jax.ShapeDtypeStruct(d_rows.shape, BF16)),
        in_specs=[vmem] * 8,
        out_specs=(vmem, vmem),
        compiler_params=pltpu.CompilerParams(vmem_limit_bytes=VMEM_LIMIT),
        name='towers_forward',
    )(q_rows, d_rows, *weights)


def score_kernel(tau_ref, q_ref, d_ref, q_up, d_up, loss_ref, q_all, d_all, st, stats, q_part, d_part, q_sum, d_sum, loss_all, send, recv):
    at = place()
    q_slot = at['y'] * SIDE + at['x']
    d_slot = at['z'] * 2 + at['core']
    q_peers = [moved(moved(at, 'x', s % SIDE), 'y', s // SIDE) for s in range(1, 16)]
    d_peers = [moved(moved(at, 'core', s % 2), 'z', s // 2) for s in range(1, 8)]

    barrier = pltpu.get_barrier_semaphore()
    for peer in q_peers + d_peers:
        pl.semaphore_signal(barrier, inc=1, device_id=device(peer), device_id_type=MESH)

    q_all[q_slot] = q_ref[...]
    d_all[d_slot] = d_ref[...]
    pl.semaphore_wait(barrier, len(q_peers) + len(d_peers))

    count = [0]
    started = []

    def copy(src, dst, peer):
        k = count[0]
        count[0] += 1
        c = pltpu.make_async_remote_copy(src_ref=src, dst_ref=dst, send_sem=send.at[k], recv_sem=recv.at[k], device_id=device(peer), device_id_type=MESH)
        c.start()
        started.append(c)
        return c

    gathers = [copy(d_ref, d_all.at[d_slot], p) for p in d_peers]
    gathers += [copy(q_ref, q_all.at[q_slot], p) for p in q_peers]
    for c in gathers:
        c.wait_recv()

    tau = tau_ref[0]
    queries = q_all[...].reshape(1024, 512)
    highs, sums = [], []
    for b in range(8):
        tile = dot(d_all[b], queries, LAST_CONTRACT) / tau
        st[b] = tile
        highs.append(jnp.max(tile, axis=0, keepdims=True))
    high = functools.reduce(jnp.maximum, highs)
    total = jnp.zeros_like(high)
    for b in range(8):
        total = total + jnp.sum(jnp.exp(st[b] - high), axis=0, keepdims=True)
    column = lax.broadcasted_iota(jnp.int32, (64, 1024), 1)
    row = lax.broadcasted_iota(jnp.int32, (64, 1024), 0)
    target = column == row + q_slot * 64
    own = st[d_slot, 0:64, :]
    positive = jnp.sum(jnp.where(target, own, 0.0), axis=0, keepdims=True)
    stats[q_slot, 0:1, :] = high
    stats[q_slot, 1:2, :] = total
    stats[q_slot, 2:3, :] = positive
    shares = [copy(stats.at[q_slot], stats.at[q_slot], p) for p in q_peers]
    for c in shares:
        c.wait_recv()
    all_stats = [stats[j] for j in range(16)]
    top = functools.reduce(jnp.maximum, [s[0:1] for s in all_stats])
    norm = sum(s[1:2] * jnp.exp(s[0:1] - top) for s in all_stats)
    log_norm = top + jnp.log(norm)
    positives = sum(s[2:3] for s in all_stats)
    part = jnp.sum(log_norm - positives, axis=1, keepdims=True)
    loss_all[d_slot] = jnp.broadcast_to(part, (8, 128))
    losses = [copy(loss_all.at[d_slot], loss_all.at[d_slot], p) for p in d_peers]

    scale = 8192.0 * tau
    d_row = lax.broadcasted_iota(jnp.int32, (128, 1024), 0)
    d_col = lax.broadcasted_iota(jnp.int32, (128, 1024), 1)
    grads = []
    for b in range(8):
        hit = (d_col == d_row + q_slot * 64) & (d_row < 64) & (d_slot == b)
        grads.append(((jnp.exp(st[b] - log_norm) - jnp.where(hit, 1.0, 0.0)) / scale).astype(BF16))
    for b in range(8):
        d_part[b] = dot(grads[b], queries)
    d_moves = [copy(d_part.at[p['z'] * 2 + p['core']], d_sum.at[d_slot], p) for p in d_peers]
    grad = jnp.concatenate(grads, axis=0)
    docs = d_all[...].reshape(1024, 512)
    q_part[...] = dot(grad, docs, ROWS_CONTRACT).reshape(16, 64, 512)
    q_moves = [copy(q_part.at[p['y'] * SIDE + p['x']], q_sum.at[q_slot], p) for p in q_peers]
    d_sum[d_slot] = d_part[d_slot]
    q_sum[q_slot] = q_part[q_slot]
    for c in losses:
        c.wait_recv()
    loss_ref[...] = sum(loss_all[j] for j in range(8)) / 8192.0
    for c in d_moves:
        c.wait_recv()
    d_up[...] = sum(d_sum[j] for j in range(8)).astype(BF16)
    for c in q_moves:
        c.wait_recv()
    q_up[...] = sum(q_sum[j] for j in range(16)).astype(BF16)
    for c in started:
        c.wait_send()


def scores(tau, q_reps, d_reps):
    vmem = pl.BlockSpec(memory_space=pltpu.VMEM)
    copies = 3 * 15 + 3 * 7
    return pl.pallas_call(
        score_kernel,
        out_shape=(
            jax.ShapeDtypeStruct((64, 512), BF16),
            jax.ShapeDtypeStruct((128, 512), BF16),
            jax.ShapeDtypeStruct((8, 128), F32),
        ),
        in_specs=[pl.BlockSpec(memory_space=pltpu.SMEM), vmem, vmem],
        out_specs=(vmem, vmem, vmem),
        scratch_shapes=[
            pltpu.VMEM((16, 64, 512), BF16),
            pltpu.VMEM((8, 128, 512), BF16),
            pltpu.VMEM((8, 128, 1024), F32),
            pltpu.VMEM((16, 3, 1024), F32),
            pltpu.VMEM((16, 64, 512), F32),
            pltpu.VMEM((8, 128, 512), F32),
            pltpu.VMEM((16, 64, 512), F32),
            pltpu.VMEM((8, 128, 512), F32),
            pltpu.VMEM((8, 8, 128), F32),
            pltpu.SemaphoreType.DMA((copies,)),
            pltpu.SemaphoreType.DMA((copies,)),
        ],
        compiler_params=pltpu.CompilerParams(collective_id=0, has_side_effects=True, vmem_limit_bytes=VMEM_LIMIT),
        name='scores',
    )(tau, q_reps, d_reps)


def gelu_back(pre, act_grad):
    return jax.vjp(jax.nn.gelu, pre)[1](act_grad)[0]


def tower_backward(sub, rows_per, x_ref, up_ref, w_one, w_two, w_proj, acc, pre_s, act_s):
    rows = pl.ds(pl.multiple_of(sub * rows_per, rows_per), rows_per)
    hidden = [x_ref[rows, :]]
    for layer in range(2):
        pre = dot(hidden[layer], w_one[layer])
        pre_s[layer, 0:rows_per] = pre
        act = jax.nn.gelu(pre).astype(BF16)
        act_s[layer, 0:rows_per] = act
        hidden.append((hidden[layer].astype(F32) + dot(act, w_two[layer])).astype(BF16))
    up = up_ref[rows, :]

    def add(base, lhs, rhs):
        for i in range(lhs.shape[1] // 256):
            part = dot(lhs[:, i * 256:(i + 1) * 256], rhs, ROWS_CONTRACT).reshape(32, 8, 512)
            at = base + i * 32
            acc[at:at + 32] += part

    add(1024, hidden[2], up)
    resid = dot(up, w_proj[...], LAST_CONTRACT)
    for layer in (1, 0):
        resid_bf = resid.astype(BF16)
        add(512 + layer * 256, act_s[layer, 0:rows_per], resid_bf)
        act_grad = dot(resid_bf, w_two[layer], LAST_CONTRACT)
        pre_grad = gelu_back(pre_s[layer, 0:rows_per], act_grad).astype(BF16)
        for c in range(4):
            add(layer * 256 + c * 64, hidden[layer], pre_grad[:, c * 512:(c + 1) * 512])
        if layer == 1:
            resid = resid + dot(pre_grad, w_one[layer], LAST_CONTRACT)


def backward_kernel(q_in, d_in, q_up, d_up, q_w1, q_w2, q_proj, d_w1, d_w2, d_proj, out, q_acc, d_acc, pre_s, act_s, sems):
    def clear(i, carry):
        q_acc[pl.ds(i * 8, 8)] = jnp.zeros((8, 8, 512), F32)
        d_acc[pl.ds(i * 8, 8)] = jnp.zeros((8, 8, 512), F32)
        return carry

    lax.fori_loop(0, UNITS // 8, clear, 0)

    def q_body(sub, carry):
        tower_backward(sub, 16, q_in, q_up, q_w1, q_w2, q_proj, q_acc, pre_s, act_s)
        return carry

    lax.fori_loop(0, SUB_COUNT, q_body, 0)
    q_copy = pltpu.make_async_copy(q_acc, out.at[0], sems.at[0])
    q_copy.start()

    def d_body(sub, carry):
        tower_backward(sub, 32, d_in, d_up, d_w1, d_w2, d_proj, d_acc, pre_s, act_s)
        return carry

    lax.fori_loop(0, SUB_COUNT, d_body, 0)
    d_copy = pltpu.make_async_copy(d_acc, out.at[1], sems.at[1])
    d_copy.start()
    q_copy.wait()
    d_copy.wait()


def backward(q_rows, d_rows, q_up, d_up, weights):
    vmem = pl.BlockSpec(memory_space=pltpu.VMEM)
    return pl.pallas_call(
        backward_kernel,
        out_shape=jax.ShapeDtypeStruct((2, UNITS, 8, 512), F32),
        in_specs=[vmem] * 10,
        out_specs=pl.BlockSpec(memory_space=pl.ANY),
        scratch_shapes=[
            pltpu.VMEM((UNITS, 8, 512), F32),
            pltpu.VMEM((UNITS, 8, 512), F32),
            pltpu.VMEM((2, 32, 2048), F32),
            pltpu.VMEM((2, 32, 2048), BF16),
            pltpu.SemaphoreType.DMA((2,)),
        ],
        compiler_params=pltpu.CompilerParams(vmem_limit_bytes=VMEM_LIMIT),
        name='towers_backward',
    )(q_rows, d_rows, q_up, d_up, *weights)


def add_into(dst, dst_at, pieces, size):
    step = next(s for s in (8, 6, 5, 4, 3, 2, 1) if size % s == 0)

    def body(i, carry):
        here = pl.ds(dst_at + i * step, step)
        total = dst[here]
        for ref, ref_at in pieces:
            total = total + ref[pl.ds(ref_at + i * step, step)]
        dst[here] = total
        return carry

    lax.fori_loop(0, size // step, body, 0)


def reduce_kernel(grads, out, mine, pair, *rest):
    bufs, (load_sem, pair_send, pair_recv, rs_send, rs_recv, ag_send, ag_recv, core_send, core_recv) = rest[:12], rest[12:]
    at = place()
    core = at['core']
    other = moved(at, 'core', 1)
    barrier = pltpu.get_barrier_semaphore()
    peers = [other] + [moved(at, d, s) for d in 'xyz' for s in (1, 3)]
    for peer in peers:
        pl.semaphore_signal(barrier, inc=1, device_id=device(peer), device_id_type=MESH)
    pl.semaphore_wait(barrier, len(peers))
    unsent = []

    def remote(src, dst, send, recv, peer):
        c = pltpu.make_async_remote_copy(src_ref=src, dst_ref=dst, send_sem=send, recv_sem=recv, device_id=device(peer), device_id_type=MESH)
        c.start()
        unsent.append(c)
        return c

    loads, pairs = {}, {}
    for rel in (2, 1, 3, 0):
        for k in range(3):
            n = 16 * COLOUR_ROWS[k]
            spot = COLOUR_OFFSET[k] + lax.rem(at[COLOUR_DIMS[k][0]] + rel, SIDE) * n
            here = pl.ds(spot, n)
            pairs[k, rel] = remote(grads.at[1 - core, here], pair.at[here], pair_send.at[k * 4 + rel], pair_recv.at[k * 4 + rel], other)
            load = pltpu.make_async_copy(grads.at[core, here], mine.at[here], load_sem.at[k * 4 + rel])
            load.start()
            loads[k, rel] = load

    def settle(k, rel):
        n = 16 * COLOUR_ROWS[k]
        spot = COLOUR_OFFSET[k] + lax.rem(at[COLOUR_DIMS[k][0]] + rel, SIDE) * n
        loads[k, rel].wait()
        pairs[k, rel].wait_recv()
        add_into(mine, spot, [(pair, spot)], n)

    base = list(COLOUR_OFFSET)

    def ring(k, p):
        dim = COLOUR_DIMS[k][p]
        n = COLOUR_ROWS[k] * (16, 4, 1)[p]
        half = (n + 1) // 2
        spot = [base[k] + lax.rem(at[dim] + rel, SIDE) * n for rel in range(4)]
        return dim, n, half, spot, moved(at, dim, 1), moved(at, dim, 3)

    moves = {}

    def rs_copy(k, p, m, src, dst, peer):
        s = (k * 3 + p) * 6 + m
        moves[k, p, m] = remote(src, dst, rs_send.at[s], rs_recv.at[s], peer)

    def rs_far(k, p):
        dim, n, half, spot, right, left = ring(k, p)
        tr = bufs[p * 4]
        tl = bufs[p * 4 + 1]
        o, oh = COLOUR_OFFSET[k] // 64 * (16, 4, 1)[p], half_offset(k, p)
        rs_copy(k, p, 0, mine.at[pl.ds(spot[2], half)], tr.at[pl.ds(oh, half)], right)
        rs_copy(k, p, 1, mine.at[pl.ds(spot[2] + half, n - half)], tl.at[pl.ds(oh, n - half)], left)

    def rs_near(k, p):
        dim, n, half, spot, right, left = ring(k, p)
        fl, fr = bufs[p * 4 + 2], bufs[p * 4 + 3]
        o = COLOUR_OFFSET[k] // 64 * (16, 4, 1)[p]
        rs_copy(k, p, 2, mine.at[pl.ds(spot[1] + half, n - half)], fl.at[pl.ds(o + half, n - half)], right)
        rs_copy(k, p, 3, mine.at[pl.ds(spot[3], half)], fr.at[pl.ds(o, half)], left)

    def rs_pass(k, p):
        dim, n, half, spot, right, left = ring(k, p)
        tr, tl, fl, fr = bufs[p * 4:p * 4 + 4]
        o, oh = COLOUR_OFFSET[k] // 64 * (16, 4, 1)[p], half_offset(k, p)
        moves[k, p, 0].wait_recv()
        add_into(mine, spot[1], [(tr, oh)], half)
        rs_copy(k, p, 4, mine.at[pl.ds(spot[1], half)], fl.at[pl.ds(o, half)], right)
        moves[k, p, 1].wait_recv()
        add_into(mine, spot[3] + half, [(tl, oh)], n - half)
        rs_copy(k, p, 5, mine.at[pl.ds(spot[3] + half, n - half)], fr.at[pl.ds(o + half, n - half)], left)

    def rs_end(k, p):
        dim, n, half, spot, right, left = ring(k, p)
        fl, fr = bufs[p * 4 + 2], bufs[p * 4 + 3]
        o = COLOUR_OFFSET[k] // 64 * (16, 4, 1)[p]
        for m in (2, 3, 4, 5):
            moves[k, p, m].wait_recv()
        add_into(mine, spot[0], [(fl, o), (fr, o)], n)
        base[k] = spot[0]

    for k in range(3):
        settle(k, 2)
        rs_far(k, 0)
    for k in range(3):
        settle(k, 1)
        settle(k, 3)
        rs_near(k, 0)
    for k in range(3):
        rs_pass(k, 0)
    for k in range(3):
        settle(k, 0)
    bases = [[] for _ in range(3)]
    for p in range(3):
        for k in range(3):
            bases[k].append(base[k])
            rs_end(k, p)
            if p < 2:
                rs_far(k, p + 1)
                rs_near(k, p + 1)
        if p < 2:
            for k in range(3):
                rs_pass(k, p + 1)

    core_moves = []
    locals_ = []

    def hand(src, spot, n):
        i = len(core_moves)
        core_moves.append(remote(src, out.at[core, pl.ds(spot, n)], core_send.at[i], core_recv.at[i], other))

    gathers = {}

    def ag_copy(k, p, m, src, spot, n, peer):
        s = (k * 3 + p) * 6 + m
        gathers[k, p, m] = remote(src, out.at[core, pl.ds(spot, n)], ag_send.at[s], ag_recv.at[s], peer)

    def ag_start(k, p):
        base[k] = bases[k][p]
        dim, n, half, spot, right, left = ring(k, p)
        src = mine if p == 2 else out.at[core]
        first = src.at[pl.ds(spot[0], half)]
        second = src.at[pl.ds(spot[0] + half, n - half)]
        ag_copy(k, p, 0, first, spot[0], half, right)
        ag_copy(k, p, 1, second, spot[0] + half, n - half, left)
        ag_copy(k, p, 2, second, spot[0] + half, n - half, right)
        ag_copy(k, p, 3, first, spot[0], half, left)

    def ag_pass(k, p):
        base[k] = bases[k][p]
        dim, n, half, spot, right, left = ring(k, p)
        gathers[k, p, 0].wait_recv()
        ag_copy(k, p, 4, out.at[core, pl.ds(spot[3], half)], spot[3], half, right)
        gathers[k, p, 1].wait_recv()
        ag_copy(k, p, 5, out.at[core, pl.ds(spot[1] + half, n - half)], spot[1] + half, n - half, left)
        gathers[k, p, 2].wait_recv()
        hand(out.at[core, pl.ds(spot[3], n)], spot[3], n)
        gathers[k, p, 3].wait_recv()
        hand(out.at[core, pl.ds(spot[1], n)], spot[1], n)

    def ag_end(k, p):
        base[k] = bases[k][p]
        dim, n, half, spot, right, left = ring(k, p)
        gathers[k, p, 4].wait_recv()
        hand(out.at[core, pl.ds(spot[2], half)], spot[2], half)
        gathers[k, p, 5].wait_recv()
        hand(out.at[core, pl.ds(spot[2] + half, n - half)], spot[2] + half, n - half)

    for k in range(3):
        n, spot = COLOUR_ROWS[k], base[k]
        ag_start(k, 2)
        hand(mine.at[pl.ds(spot, n)], spot, n)
        local = pltpu.make_async_copy(mine.at[pl.ds(spot, n)], out.at[core, pl.ds(spot, n)], load_sem.at[12 + k])
        local.start()
        locals_.append(local)
    for p in (2, 1, 0):
        for k in range(3):
            ag_pass(k, p)
        for k in range(3):
            ag_end(k, p)
            if p == 2:
                locals_[k].wait()
            if p > 0:
                ag_start(k, p - 1)
    for c in core_moves:
        c.wait_recv()
    for c in unsent:
        c.wait_send()


def half_offset(k, p):
    sizes = [(r * (16, 4, 1)[p] + 1) // 2 for r in COLOUR_ROWS]
    return sum(sizes[:k])


def all_reduce(grads):
    scale = (16, 4, 1)
    bufs = []
    for p in range(3):
        halves = sum((r * scale[p] + 1) // 2 for r in COLOUR_ROWS)
        full = sum(COLOUR_ROWS) * scale[p]
        bufs += [pltpu.VMEM((n, 8, 512), F32) for n in (halves, halves, full, full)]
    dma = pltpu.SemaphoreType.DMA
    return pl.pallas_call(
        reduce_kernel,
        out_shape=jax.ShapeDtypeStruct(grads.shape, F32),
        in_specs=[pl.BlockSpec(memory_space=pl.ANY)],
        out_specs=pl.BlockSpec(memory_space=pl.ANY),
        scratch_shapes=[pltpu.VMEM((UNITS, 8, 512), F32), pltpu.VMEM((UNITS, 8, 512), F32)] + bufs
        + [dma((15,)), dma((12,)), dma((12,)), dma((54,)), dma((54,)), dma((54,)), dma((54,)), dma((39,)), dma((39,))],
        compiler_params=pltpu.CompilerParams(collective_id=1, has_side_effects=True, vmem_limit_bytes=VMEM_LIMIT),
        name='all_reduce',
    )(grads)


def unpack(total):
    w_one = total[:512].reshape(2, 4, 512, 512).transpose(0, 2, 1, 3).reshape(2, 512, 2048)
    w_two = total[512:1024].reshape(2, 2048, 512)
    return w_one, w_two, total[1024:].reshape(512, 512)


def local_step(q_loc, d_loc, temperature, *weights):
    d_rows = d_loc.reshape(-1, d_loc.shape[-1])
    q_reps, d_reps = forward(q_loc, d_rows, weights)
    q_up, d_up, loss = scores(temperature.reshape(1), q_reps, d_reps)
    total = all_reduce(backward(q_loc, d_rows, q_up, d_up, weights))
    return (loss[0, 0], *unpack(total[0]), *unpack(total[1]))


def solution(mesh):
    specs_in = (P('data', None), P(None, 'data', None), P(), P(), P(), P(), P(), P(), P())
    specs_out = (P(), P(), P(), P(), P(), P(), P())
    return jax.shard_map(local_step, mesh=mesh, in_specs=specs_in, out_specs=specs_out, check_vma=False)
```

```python
import functools

import jax
import jax.numpy as jnp
from jax import lax
from jax.experimental import pallas as pl
from jax.experimental.pallas import tpu as pltpu
from jax.sharding import PartitionSpec as P

F32 = jnp.float32
BF16 = jnp.bfloat16
MESH = pl.DeviceIdType.MESH
SUB_COUNT = 4
SIDE = 4
ROWS_CONTRACT = (((0,), (0,)), ((), ()))
LAST_CONTRACT = (((1,), (1,)), ((), ()))
VMEM_LIMIT = 67043328

UNITS = 2176
HALF = 1088
TRAIN_VMEM = 27500000
PAIR_SLOT = (1, 1, 0, 0)
RING_SIZE = (16, 4, 1)
Q, D = range(2)
OUTER, MIDDLE, INNER = range(3)
OWN, RIGHT, ACROSS, LEFT = range(4)
MESSAGES = (
    (ACROSS, False, 0, 0), (ACROSS, True, 1, 0), (RIGHT, True, 0, 1), (LEFT, False, 1, 2), (RIGHT, False, 0, 1), (LEFT, True, 1, 2),
    (OWN, False, 0, None), (OWN, True, 1, None), (OWN, True, 0, None), (OWN, False, 1, None), (LEFT, False, 0, None), (RIGHT, True, 1, None),
)
ALL = tuple(range(len(MESSAGES)))
FAR, NEAR, ON, GATHER = ALL[:2], ALL[2:4], ALL[4:6], ALL[6:]
FIRST, SECOND, ONWARD = GATHER[:2], GATHER[2:4], GATHER[4:]
COLOURS = ((0, 6, ('x', 'y', 'z')), (384, 6, ('y', 'z', 'x')), (768, 5, ('z', 'x', 'y')))
HANDS = ((LEFT, False), (RIGHT, False), (ACROSS, False), (ACROSS, True), (OWN, False))


def place():
    me = lax.axis_index('data')
    core = lax.rem(me, 2)
    x = lax.rem(me // 2, SIDE)
    y = lax.rem(me // 8, SIDE)
    z = me // 32
    return dict(z=z, y=y, x=x, core=core)


def device(at):
    return (((at['z'] * SIDE + at['y']) * SIDE + at['x']) * 2 + at['core'],)


def moved(at, dim, step):
    size = 2 if dim == 'core' else SIDE
    return {**at, dim: lax.rem(at[dim] + step, size)}


def remote(src, dst, sems, index, peer):
    return pltpu.make_async_remote_copy(
        src_ref=src, dst_ref=dst, send_sem=sems[0].at[index], recv_sem=sems[1].at[index], device_id=device(peer), device_id_type=MESH
    )


def greet(peers):
    for peer in peers:
        pl.semaphore_signal(pltpu.get_barrier_semaphore(), inc=1, device_id=device(peer), device_id_type=MESH)


def dot(lhs, rhs, dims=None):
    if dims is None:
        return jnp.dot(lhs, rhs, preferred_element_type=F32)
    return lax.dot_general(lhs, rhs, dims, preferred_element_type=F32)


def add_into(dst, dst_at, pieces, size):
    step = next(s for s in (16, 12, 10, 8, 6, 5, 4, 3, 2, 1) if size % s == 0)

    def body(i, carry):
        here = pl.ds(dst_at + i * step, step)
        total = dst[here]
        for ref, ref_at in pieces:
            total = total + ref[pl.ds(ref_at + i * step, step)]
        dst[here] = total
        return carry

    lax.fori_loop(0, size // step, body, 0)


class Ring:
    def __init__(self, at, dim, x, base, n, buf, buf_at, sems, sem_at):
        self.x, self.n, self.buf, self.buf_at = x, n, buf, buf_at
        self.half = (n + 1) // 2
        self.rest = n - self.half
        self.spot = [base + lax.rem(at[dim] + rel, SIDE) * n for rel in range(SIDE)]
        self.peers = moved(at, dim, RIGHT), moved(at, dim, LEFT)
        self.sems, self.sem_at = sems, sem_at * len(MESSAGES)

    def copy(self, m):
        rel, second, way, slot = MESSAGES[m]
        shift, size = (self.half, self.rest) if second else (0, self.half)
        src = self.x.at[pl.ds(self.spot[rel] + shift, size)]
        dst = src if slot is None else self.buf.at[pl.ds(self.buf_at + slot * self.n + shift, size)]
        return remote(src, dst, self.sems, self.sem_at + m, self.peers[way])

    def start(self, which):
        for m in which:
            self.copy(m).start()

    def take(self, which):
        for m in which:
            self.copy(m).wait_recv()

    def sent(self, which):
        for m in which:
            self.copy(m).wait_send()

    def rs_pass(self):
        self.take(FAR[:1])
        add_into(self.x, self.spot[RIGHT], [(self.buf, self.buf_at)], self.half)
        self.start(ON[:1])
        self.take(FAR[1:])
        add_into(self.x, self.spot[LEFT] + self.half, [(self.buf, self.buf_at + self.half)], self.rest)
        self.start(ON[1:])

    def rs_end(self):
        self.take(NEAR + ON)
        got = [(self.buf, self.buf_at + slot * self.n) for slot in (1, 2)]
        add_into(self.x, self.spot[OWN], got, self.n)

    def ag_pass(self):
        for first, then in zip(GATHER[:2], GATHER[4:]):
            self.copy(first).wait_recv()
            self.copy(then).start()


def tower_forward(rows, w_one, w_two, w_proj):
    hidden = rows
    for layer in range(2):
        act = jax.nn.gelu(dot(hidden, w_one[layer])).astype(BF16)
        hidden = (hidden.astype(F32) + dot(act, w_two[layer])).astype(BF16)
    return dot(hidden, w_proj[...]).astype(BF16)


def forward_kernel(q_in, d_in, q_w1, q_w2, q_proj, d_w1, d_w2, d_proj, q_out, d_out):
    def body(sub, carry):
        rows = pl.ds(pl.multiple_of(sub * 16, 16), 16)
        q_out[rows, :] = tower_forward(q_in[rows, :], q_w1, q_w2, q_proj)
        rows = pl.ds(pl.multiple_of(sub * 32, 32), 32)
        d_out[rows, :] = tower_forward(d_in[rows, :], d_w1, d_w2, d_proj)
        return carry

    lax.fori_loop(0, SUB_COUNT, body, 0)


def forward(q_rows, d_rows, weights):
    vmem = pl.BlockSpec(memory_space=pltpu.VMEM)
    return pl.pallas_call(
        forward_kernel,
        out_shape=(jax.ShapeDtypeStruct(q_rows.shape, BF16), jax.ShapeDtypeStruct(d_rows.shape, BF16)),
        in_specs=[vmem] * 8,
        out_specs=(vmem, vmem),
        compiler_params=pltpu.CompilerParams(vmem_limit_bytes=VMEM_LIMIT),
        name='towers_forward',
    )(q_rows, d_rows, *weights)


def score_kernel(tau_ref, q_ref, d_ref, q_up, d_up, loss_ref, q_all, d_all, st, stats, q_part, d_part, q_buf, d_buf, pair, loss_all, *sems):
    at = place()
    core, z = at['core'], at['z']
    other = moved(at, 'core', 1)
    q_peers = [moved(moved(at, 'x', s % SIDE), 'y', s // SIDE) for s in range(1, 16)]
    d_peers = [moved(moved(at, 'core', s % 2), 'z', s // 2) for s in range(1, 8)]
    q_slot, d_slot = at['y'] * SIDE + at['x'], core * SIDE + z
    greet(q_peers + d_peers)

    outer, inner = ('y', 'x'), ('x', 'y')
    own = [at[outer[h]] * 8 + at[inner[h]] * 2 for h in range(2)]
    for h in range(2):
        q_all[h, pl.ds(own[h], 2)] = q_ref[h * 32:(h + 1) * 32, :].reshape(2, 16, 512)
    d_all[core, pl.ds(z * 8, 8)] = d_ref[...].reshape(8, 16, 512)

    def q_rings(x, h):
        wide = Ring(at, outer[h], x.at[h], 0, 8, q_buf.at[h], 0, sems, h)
        return wide, Ring(at, inner[h], x.at[h], at[outer[h]] * 8, 2, q_buf.at[h], 24, sems, 2 + h)

    q_wide, q_thin = zip(*[q_rings(q_all, h) for h in range(2)])
    docs_ring = Ring(at, 'z', d_all.at[core], 0, 8, d_buf, 0, sems, 4)
    hands_at = 5 * len(MESSAGES)
    pl.semaphore_wait(pltpu.get_barrier_semaphore(), len(q_peers) + len(d_peers))

    def hand(rel):
        here = d_all.at[core, pl.ds(docs_ring.spot[rel], 8)]
        return remote(here, here, sems, hands_at + rel, other)

    docs_ring.start(FIRST + SECOND)
    hand(OWN).start()
    for ring in q_thin:
        ring.start(FIRST + SECOND)
    for ring in q_thin:
        ring.ag_pass()
    docs_ring.ag_pass()
    for thin, wide in zip(q_thin, q_wide):
        thin.take(SECOND + ONWARD)
        wide.start(FIRST + SECOND)
    docs_ring.take(SECOND)
    hand(LEFT).start()
    hand(RIGHT).start()
    docs_ring.take(ONWARD)
    hand(ACROSS).start()
    for ring in q_wide:
        ring.ag_pass()
    for rel in range(SIDE):
        hand(rel).wait_recv()
    for ring in q_wide:
        ring.take(SECOND + ONWARD)

    tau = tau_ref[0]
    queries = q_all[...].reshape(1024, 512)
    blocks = [(c, j) for c in range(2) for j in range(SIDE)]

    def block(ref, c, j):
        return ref[c, j * 8:(j + 1) * 8].reshape(128, 512)

    highs = []
    for b, (c, j) in enumerate(blocks):
        tile = dot(block(d_all, c, j), queries, LAST_CONTRACT) / tau
        st[b] = tile
        highs.append(jnp.max(tile, axis=0, keepdims=True))
    high = functools.reduce(jnp.maximum, highs)
    total = sum(jnp.sum(jnp.exp(st[b] - high), axis=0, keepdims=True) for b in range(len(blocks)))

    def matches(rows):
        row = lax.broadcasted_iota(jnp.int32, (rows, 1024), 0)
        column = lax.broadcasted_iota(jnp.int32, (rows, 1024), 1)
        return (row < 64) & (column == jnp.where(row < 32, own[0] * 16 + row, 480 + own[1] * 16 + row))

    positive = jnp.sum(jnp.where(matches(64), st[d_slot, 0:64, :], 0.0), axis=0, keepdims=True)
    for i, row in enumerate((high, total, positive)):
        stats[q_slot, i:i + 1, :] = row
    extra = hands_at + SIDE
    shares = [remote(stats.at[q_slot], stats.at[q_slot], sems, extra + i, p) for i, p in enumerate(q_peers)]
    for c in shares:
        c.start()
    for c in shares:
        c.wait_recv()
    all_stats = [stats[j] for j in range(16)]
    top = functools.reduce(jnp.maximum, [s[0:1] for s in all_stats])
    norm = sum(s[1:2] * jnp.exp(s[0:1] - top) for s in all_stats)
    log_norm = top + jnp.log(norm)
    part = jnp.sum(log_norm - sum(s[2:3] for s in all_stats), axis=1, keepdims=True)
    loss_all[d_slot] = jnp.broadcast_to(part, (8, 128))
    extra = extra + len(shares)
    losses = [remote(loss_all.at[d_slot], loss_all.at[d_slot], sems, extra + i, p) for i, p in enumerate(d_peers)]
    for c in losses:
        c.start()

    scale = 8192.0 * tau
    hit = matches(128)
    grads = []
    for b in range(len(blocks)):
        soft = jnp.exp(st[b] - log_norm) - jnp.where(hit & (d_slot == b), 1.0, 0.0)
        grads.append((soft / scale).astype(BF16))
    grad = jnp.concatenate(grads, axis=0)
    docs = d_all[...].reshape(1024, 512)
    q_wide, q_thin = zip(*[q_rings(q_part, h) for h in range(2)])
    for h in range(2):
        q_part[h] = dot(grad[:, h * 512:(h + 1) * 512], docs, ROWS_CONTRACT).reshape(32, 16, 512)
        q_wide[h].start(FAR + NEAR)

    extra = extra + len(losses)
    for b, (c, j) in enumerate(blocks):
        d_part[c, j * 8:(j + 1) * 8] = dot(grads[b], queries).reshape(8, 16, 512)
    swap = remote(d_part.at[other['core']], pair, sems, extra, other)
    swap.start()
    docs_sum = Ring(at, 'z', d_part.at[core], 0, 8, d_buf, 0, sems, 4)
    q_wide[0].rs_pass()
    swap.wait_recv()
    add_into(d_part.at[core], 0, [(pair, 0)], 32)
    docs_sum.start(FAR + NEAR)
    q_wide[1].rs_pass()
    for wide, thin in zip(q_wide, q_thin):
        wide.rs_end()
        thin.start(FAR + NEAR)
    docs_sum.rs_pass()
    for ring in q_thin:
        ring.rs_pass()
    for c in losses:
        c.wait_recv()
    loss_ref[...] = sum(loss_all[j] for j in range(8)) / 8192.0
    for h, ring in enumerate(q_thin):
        ring.rs_end()
        q_up[h * 32:(h + 1) * 32, :] = q_part[h, pl.ds(own[h], 2)].reshape(32, 512).astype(BF16)
    docs_sum.rs_end()
    d_up[...] = d_part[core, pl.ds(z * 8, 8)].reshape(128, 512).astype(BF16)
    for c in shares + losses + [swap] + list(map(hand, range(SIDE))):
        c.wait_send()
    for ring in (*q_wide, *q_thin, docs_sum):
        ring.sent(FAR + NEAR + ON)
    for h in range(2):
        for ring in q_rings(q_all, h):
            ring.sent(GATHER)
    docs_ring.sent(GATHER)


def scores(tau, q_reps, d_reps):
    vmem = pl.BlockSpec(memory_space=pltpu.VMEM)
    copies = 5 * len(MESSAGES) + 27
    return pl.pallas_call(
        score_kernel,
        out_shape=tuple(jax.ShapeDtypeStruct(*s) for s in (((64, 512), BF16), ((128, 512), BF16), ((8, 128), F32))),
        in_specs=[pl.BlockSpec(memory_space=pltpu.SMEM), vmem, vmem],
        out_specs=(vmem,) * 3,
        scratch_shapes=[
            pltpu.VMEM((2, 32, 16, 512), BF16),
            pltpu.VMEM((2, 32, 16, 512), BF16),
            pltpu.VMEM((8, 128, 1024), F32),
            pltpu.VMEM((16, 3, 1024), F32),
            pltpu.VMEM((2, 32, 16, 512), F32),
            pltpu.VMEM((2, 32, 16, 512), F32),
            pltpu.VMEM((2, 30, 16, 512), F32),
            pltpu.VMEM((24, 16, 512), F32),
            pltpu.VMEM((32, 16, 512), F32),
            pltpu.VMEM((8, 8, 128), F32),
            pltpu.SemaphoreType.DMA((copies,)),
            pltpu.SemaphoreType.DMA((copies,)),
        ],
        compiler_params=pltpu.CompilerParams(collective_id=0, has_side_effects=True, vmem_limit_bytes=VMEM_LIMIT),
        name='scores',
    )(tau, q_reps, d_reps)


def gelu_back(pre, act_grad):
    return jax.vjp(jax.nn.gelu, pre)[1](act_grad)[0]


def tower_backward(sub, rows_per, x_ref, up_ref, w_one, w_two, w_proj, acc, pre_s, act_s):
    rows = pl.ds(pl.multiple_of(sub * rows_per, rows_per), rows_per)
    hidden = [x_ref[rows, :]]
    for layer in range(2):
        pre = dot(hidden[layer], w_one[layer])
        pre_s[layer, 0:rows_per] = pre
        act = jax.nn.gelu(pre).astype(BF16)
        act_s[layer, 0:rows_per] = act
        hidden.append((hidden[layer].astype(F32) + dot(act, w_two[layer])).astype(BF16))
    up = up_ref[rows, :]

    def add(base, stride, lhs, rhs):
        for i in range(lhs.shape[1] // 256):
            part = dot(lhs[:, i * 256:(i + 1) * 256], rhs, ROWS_CONTRACT)
            for j in range(2):
                spot = base + j * stride + i * 32
                acc[spot:spot + 32] += part[:, j * 256:(j + 1) * 256].reshape(32, 8, 256)

    add(2048, 64, hidden[2], up)
    resid = dot(up, w_proj[...], LAST_CONTRACT)
    for layer in (1, 0):
        resid_bf = resid.astype(BF16)
        add(1024 + layer * 512, 256, act_s[layer, 0:rows_per], resid_bf)
        act_grad = dot(resid_bf, w_two[layer], LAST_CONTRACT)
        pre_grad = gelu_back(pre_s[layer, 0:rows_per], act_grad).astype(BF16)
        for c in range(4):
            add(layer * 512 + c * 128, 64, hidden[layer], pre_grad[:, c * 512:(c + 1) * 512])
        if layer == 1:
            resid = resid + dot(pre_grad, w_one[layer], LAST_CONTRACT)


class Exchange:
    def __init__(self, acc, pair, bufs, sems):
        self.acc, self.pair = acc, pair
        self.pair_sems, self.ring_sems, self.hand_sems, self.credit, self.ready = sems[:2], sems[2:4], sems[4:6], sems[6], sems[7]
        self.at = place()
        self.core = self.at['core']
        self.other = moved(self.at, 'core', 1)
        self.around = [moved(self.at, d, s) for d in 'xyz' for s in (LEFT, RIGHT)]
        greet([self.other] + self.around)
        self.rings = {}
        for t in (Q, D):
            for k, (first, rows, dims) in enumerate(COLOURS):
                base = self.core * HALF + first
                for p in (OUTER, MIDDLE, INNER):
                    n = rows * RING_SIZE[p]
                    index = (t * len(COLOURS) + k) * len(RING_SIZE) + p
                    self.rings[t, k, p] = Ring(self.at, dims[p], acc.at[t], base, n, bufs[p], 3 * first // SIDE ** (p + 1), self.ring_sems, index)
                    base = base + self.at[dims[p]] * n

    def met(self):
        pl.semaphore_wait(pltpu.get_barrier_semaphore(), len(self.around) + 1)

    def level(self, t, p):
        return [self.rings[t, k, p] for k in range(len(COLOURS))]

    def pair_copy(self, t, rel, k):
        first, ring = COLOURS[k][0], self.rings[t, k, OUTER]
        spot = ring.spot[rel] + (1 - self.core * 2) * HALF
        dst = self.pair.at[PAIR_SLOT[rel], pl.ds(first // SIDE, ring.n)]
        return remote(self.acc.at[t, pl.ds(spot, ring.n)], dst, self.pair_sems, t * 12 + rel * 3 + k, self.other)

    def pairs(self, t, rel, fresh=False):
        if not fresh:
            pl.semaphore_wait(self.credit.at[PAIR_SLOT[rel]], 1)
        for k in range(len(COLOURS)):
            self.pair_copy(t, rel, k).start()

    def settle(self, t, rel, last=False):
        for k, ring in enumerate(self.level(t, OUTER)):
            self.pair_copy(t, rel, k).wait_recv()
            add_into(ring.x, ring.spot[rel], [(self.pair.at[PAIR_SLOT[rel]], COLOURS[k][0] // SIDE)], ring.n)
        if not last:
            pl.semaphore_signal(self.credit.at[PAIR_SLOT[rel]], inc=1, device_id=device(self.other), device_id_type=MESH)

    def start(self, t, p, which):
        for ring in self.level(t, p):
            ring.start(which)

    def rs_pass(self, t, p):
        for ring in self.level(t, p):
            ring.rs_pass()

    def rs_end(self, t, p):
        for ring in self.level(t, p):
            ring.rs_end()
        for k, ring in enumerate(self.level(t, p)):
            ring.sent(FAR + NEAR + ON)
            for rel in range(SIDE) if p == OUTER else ():
                self.pair_copy(t, rel, k).wait_send()
        for peer in self.around:
            pl.semaphore_signal(self.ready.at[t * 3 + p], inc=1, device_id=device(peer), device_id_type=MESH)
        if p == OUTER:
            pl.semaphore_signal(self.ready.at[6 + t], inc=1, device_id=device(self.other), device_id_type=MESH)

    def opened(self, t, p):
        pl.semaphore_wait(self.ready.at[t * 3 + p], len(self.around))

    def hand(self, t, k, p, rel, second):
        ring = self.rings[t, k, p]
        shift, size = (0, ring.n) if rel != ACROSS else (ring.half, ring.rest) if second else (0, ring.half)
        here = self.acc.at[t, pl.ds(ring.spot[rel] + shift, size)]
        kind = HANDS.index((rel, second))
        return remote(here, here, self.hand_sems, ((t * 3 + k) * 3 + p) * len(HANDS) + kind, self.other)

    def ag_start(self, t, p, which=FIRST + SECOND):
        self.start(t, p, which)
        if p == INNER:
            pl.semaphore_wait(self.ready.at[6 + t], 1)
            for k in range(len(COLOURS)):
                self.hand(t, k, p, OWN, False).start()

    def ag_pass(self, t, p):
        for ring in self.level(t, p):
            ring.ag_pass()
        for k, ring in enumerate(self.level(t, p)):
            for m, rel in zip(SECOND, (LEFT, RIGHT)):
                ring.take((m,))
                self.hand(t, k, p, rel, False).start()

    def ag_end(self, t, p):
        for k, ring in enumerate(self.level(t, p)):
            for m, second in zip(ONWARD, (False, True)):
                ring.take((m,))
                self.hand(t, k, p, ACROSS, second).start()

    def finish(self):
        hands = [(t, k, p, *h) for t, k, p in self.rings for h in HANDS if h[0] != OWN or p == INNER]
        for h in hands:
            self.hand(*h).wait_recv()
        for ring in self.rings.values():
            ring.sent(GATHER)
        for h in hands:
            self.hand(*h).wait_send()


def train_kernel(q_in, d_in, q_up, d_up, q_w1, q_w2, q_proj, d_w1, d_w2, d_proj, acc, w_one, w_two, w_proj, pre_s, act_s, pair, *rest):
    bufs, w_sems, sems = rest[:3], rest[3], rest[4:]
    ex = Exchange(acc, pair, bufs, sems)

    def load(refs):
        return [pltpu.make_async_copy(src, dst, w_sems.at[i]) for i, (src, dst) in enumerate(zip(refs, (w_one, w_two, w_proj)))]

    def clear(t):
        def body(i, carry):
            acc[t, pl.ds(i * 16, 16)] = jnp.zeros((16, 8, 256), F32)
            return carry

        lax.fori_loop(0, UNITS // 16, body, 0)

    loads = load((q_w1, q_w2, q_proj))
    for c in loads:
        c.start()
    clear(Q)
    for c in loads:
        c.wait()

    def q_body(sub, carry):
        tower_backward(sub, 16, q_in, q_up, w_one, w_two, w_proj, acc.at[Q], pre_s, act_s)
        return carry

    lax.fori_loop(0, SUB_COUNT, q_body, 0)
    ex.met()
    ex.pairs(Q, ACROSS, fresh=True)
    ex.pairs(Q, RIGHT, fresh=True)
    loads = load((d_w1, d_w2, d_proj))
    for c in loads:
        c.start()
    clear(D)
    ex.settle(Q, ACROSS)
    ex.start(Q, OUTER, FAR)
    ex.pairs(Q, LEFT)
    ex.settle(Q, RIGHT)
    ex.pairs(Q, OWN)
    for c in loads:
        c.wait()

    def d_body(sub, carry):
        tower_backward(sub, 32, d_in, d_up, w_one, w_two, w_proj, acc.at[D], pre_s, act_s)

        @pl.when(sub == 0)
        def _():
            ex.settle(Q, LEFT)
            ex.start(Q, OUTER, NEAR)
            ex.settle(Q, OWN)

        @pl.when(sub == 1)
        def _():
            ex.rs_pass(Q, OUTER)

        return carry

    lax.fori_loop(0, SUB_COUNT, d_body, 0)
    ex.pairs(D, ACROSS)
    ex.pairs(D, RIGHT)
    ex.rs_end(Q, OUTER)
    ex.start(Q, MIDDLE, FAR + NEAR)
    ex.settle(D, ACROSS)
    ex.pairs(D, LEFT)
    ex.rs_pass(Q, MIDDLE)
    ex.settle(D, RIGHT)
    ex.pairs(D, OWN)
    ex.rs_end(Q, MIDDLE)
    ex.start(Q, INNER, FAR + NEAR)
    ex.opened(Q, OUTER)
    ex.start(D, OUTER, FAR)
    ex.settle(D, LEFT, last=True)
    ex.rs_pass(Q, INNER)
    ex.start(D, OUTER, NEAR)
    ex.settle(D, OWN, last=True)
    ex.rs_end(Q, INNER)
    ex.opened(Q, INNER)
    ex.ag_start(Q, INNER)
    ex.rs_pass(D, OUTER)
    ex.ag_pass(Q, INNER)
    ex.ag_end(Q, INNER)
    ex.opened(Q, MIDDLE)
    ex.ag_start(Q, MIDDLE)
    ex.ag_pass(Q, MIDDLE)
    ex.rs_end(D, OUTER)
    ex.start(D, MIDDLE, FAR + NEAR)
    ex.ag_end(Q, MIDDLE)
    ex.ag_start(Q, OUTER, FIRST)
    ex.rs_pass(D, MIDDLE)
    ex.rs_end(D, MIDDLE)
    ex.start(D, INNER, FAR + NEAR)
    ex.ag_start(Q, OUTER, SECOND)
    ex.rs_pass(D, INNER)
    ex.rs_end(D, INNER)
    ex.opened(D, INNER)
    ex.ag_start(D, INNER)
    ex.ag_pass(Q, OUTER)
    ex.ag_pass(D, INNER)
    ex.ag_end(D, INNER)
    ex.opened(D, MIDDLE)
    ex.ag_start(D, MIDDLE)
    ex.ag_end(Q, OUTER)
    ex.ag_pass(D, MIDDLE)
    ex.ag_end(D, MIDDLE)
    ex.opened(D, OUTER)
    ex.ag_start(D, OUTER)
    ex.ag_pass(D, OUTER)
    ex.ag_end(D, OUTER)
    ex.finish()


def train(q_rows, d_rows, q_up, d_up, weights):
    vmem, whole = pl.BlockSpec(memory_space=pltpu.VMEM), pl.BlockSpec(memory_space=pl.ANY)
    bufs = [pltpu.VMEM((3 * HALF // SIDE ** p // SIDE, 8, 256), F32) for p in (OUTER, MIDDLE, INNER)]
    dma = pltpu.SemaphoreType.DMA
    return pl.pallas_call(
        train_kernel,
        out_shape=pltpu.VMEM((2, UNITS, 8, 256), F32),
        in_specs=[vmem] * 4 + [whole] * 6,
        out_specs=vmem,
        scratch_shapes=[
            pltpu.VMEM((2, 512, 2048), BF16),
            pltpu.VMEM((2, 2048, 512), BF16),
            pltpu.VMEM((512, 512), BF16),
            pltpu.VMEM((2, 32, 2048), F32),
            pltpu.VMEM((2, 32, 2048), BF16),
            pltpu.VMEM((2, 272, 8, 256), F32),
            *bufs,
            dma((3,)), *[dma((n,)) for n in (24, 24, 216, 216, 90, 90)],
            pltpu.SemaphoreType.REGULAR((2,)), pltpu.SemaphoreType.REGULAR((8,)),
        ],
        compiler_params=pltpu.CompilerParams(collective_id=1, has_side_effects=True, vmem_limit_bytes=TRAIN_VMEM),
        name='towers_backward_all_reduce',
    )(q_rows, d_rows, q_up, d_up, *weights)


def unpack_kernel(acc, *rest):
    outs, sem = rest[:6], rest[6]
    copies = []
    for t in range(2):
        one, two, proj = outs[t * 3:t * 3 + 3]
        for k in range(2):
            for c in range(8):
                copies.append((acc.at[t, pl.ds(k * 512 + c * 64, 64)], one.at[k, :, :, pl.ds(c * 256, 256)]))
            for c in range(2):
                copies.append((acc.at[t, pl.ds(1024 + k * 512 + c * 256, 256)], two.at[k, :, :, pl.ds(c * 256, 256)]))
        for c in range(2):
            copies.append((acc.at[t, pl.ds(2048 + c * 64, 64)], proj.at[:, :, pl.ds(c * 256, 256)]))
    copies = [pltpu.make_async_copy(src, dst, sem.at[i]) for i, (src, dst) in enumerate(copies)]
    for c in copies:
        c.start()
    for c in copies:
        c.wait()


def unpack(acc):
    shapes = ((2, 64, 8, 2048), (2, 256, 8, 512), (64, 8, 512)) * 2
    outs = pl.pallas_call(
        unpack_kernel,
        out_shape=tuple(jax.ShapeDtypeStruct(s, F32) for s in shapes),
        in_specs=[pl.BlockSpec(memory_space=pltpu.VMEM)],
        out_specs=(pl.BlockSpec(memory_space=pl.ANY),) * 6,
        scratch_shapes=[pltpu.SemaphoreType.DMA((44,))],
        compiler_params=pltpu.CompilerParams(vmem_limit_bytes=1 << 20),
        name='unpack',
    )(acc)
    final = ((2, 512, 2048), (2, 2048, 512), (512, 512)) * 2
    return tuple(o.reshape(s) for o, s in zip(outs, final))


def local_step(q_loc, d_loc, temperature, *weights):
    d_rows = d_loc.reshape(-1, d_loc.shape[-1])
    q_reps, d_reps = forward(q_loc, d_rows, weights)
    q_up, d_up, loss = scores(temperature.reshape(1), q_reps, d_reps)
    return (loss[0, 0], *unpack(train(q_loc, d_rows, q_up, d_up, weights)))


def solution(mesh):
    specs_in = (P('data', None), P(None, 'data', None), P(), P(), P(), P(), P(), P(), P())
    specs_out = (P(), P(), P(), P(), P(), P(), P())
    return jax.shard_map(local_step, mesh=mesh, in_specs=specs_in, out_specs=specs_out, check_vma=False)
```

```python
import functools

import jax
import jax.numpy as jnp
from jax import lax
from jax.experimental import pallas as pl
from jax.experimental.pallas import tpu as pltpu
from jax.sharding import PartitionSpec as P

F32 = jnp.float32
BF16 = jnp.bfloat16
MESH = pl.DeviceIdType.MESH
SUB_COUNT = 4
SIDE = 4
ROWS_CONTRACT = (((0,), (0,)), ((), ()))
LAST_CONTRACT = (((1,), (1,)), ((), ()))
VMEM_LIMIT = 67043328

UNITS = 2176
HALF = 1088
TRAIN_VMEM = 27500000
PAIR_SLOT = (1, 1, 0, 0)
RING_SIZE = (16, 4, 1)
Q, D = range(2)
OUTER, MIDDLE, INNER = range(3)
OWN, RIGHT, ACROSS, LEFT = range(4)
MESSAGES = (
    (ACROSS, False, 0, 0), (ACROSS, True, 1, 0), (RIGHT, True, 0, 1), (LEFT, False, 1, 2), (RIGHT, False, 0, 1), (LEFT, True, 1, 2),
    (OWN, False, 0, None), (OWN, True, 1, None), (OWN, True, 0, None), (OWN, False, 1, None), (LEFT, False, 0, None), (RIGHT, True, 1, None),
)
ALL = tuple(range(len(MESSAGES)))
FAR, NEAR, ON, GATHER = ALL[:2], ALL[2:4], ALL[4:6], ALL[6:]
FIRST, SECOND, ONWARD = GATHER[:2], GATHER[2:4], GATHER[4:]
DIM, FFN, COLS = 512, 2048, 256
WEIGHT_SHAPES = ((2, DIM, FFN), (2, FFN, DIM), (DIM, DIM))
COLOURS = ((0, 6, ('x', 'y', 'z')), (384, 6, ('y', 'z', 'x')), (768, 5, ('z', 'x', 'y')))
HANDS = ((LEFT, False), (RIGHT, False), (ACROSS, False), (ACROSS, True), (OWN, False))


def place():
    me = lax.axis_index('data')
    core = lax.rem(me, 2)
    x = lax.rem(me // 2, SIDE)
    y = lax.rem(me // 8, SIDE)
    z = me // 32
    return dict(z=z, y=y, x=x, core=core)


def device(at):
    return (((at['z'] * SIDE + at['y']) * SIDE + at['x']) * 2 + at['core'],)


def moved(at, dim, step):
    size = 2 if dim == 'core' else SIDE
    return {**at, dim: lax.rem(at[dim] + step, size)}


def remote(src, dst, sems, index, peer):
    return pltpu.make_async_remote_copy(
        src_ref=src, dst_ref=dst, send_sem=sems[0].at[index], recv_sem=sems[1].at[index], device_id=device(peer), device_id_type=MESH
    )


def greet(peers):
    for peer in peers:
        pl.semaphore_signal(pltpu.get_barrier_semaphore(), inc=1, device_id=device(peer), device_id_type=MESH)


def dot(lhs, rhs, dims=None):
    if dims is None:
        return jnp.dot(lhs, rhs, preferred_element_type=F32)
    return lax.dot_general(lhs, rhs, dims, preferred_element_type=F32)


def add_into(dst, dst_at, pieces, size):
    step = next(s for s in (16, 12, 10, 8, 6, 5, 4, 3, 2, 1) if size % s == 0)

    def body(i, carry):
        here = pl.ds(dst_at + i * step, step)
        total = dst[here]
        for ref, ref_at in pieces:
            total = total + ref[pl.ds(ref_at + i * step, step)]
        dst[here] = total
        return carry

    lax.fori_loop(0, size // step, body, 0)


class Ring:
    def __init__(self, at, dim, x, base, n, buf, buf_at, sems, sem_at):
        self.x, self.n, self.buf, self.buf_at = x, n, buf, buf_at
        self.half = (n + 1) // 2
        self.rest = n - self.half
        self.spot = [base + lax.rem(at[dim] + rel, SIDE) * n for rel in range(SIDE)]
        self.peers = moved(at, dim, RIGHT), moved(at, dim, LEFT)
        self.sems, self.sem_at = sems, sem_at * len(MESSAGES)

    def copy(self, m):
        rel, second, way, slot = MESSAGES[m]
        shift, size = (self.half, self.rest) if second else (0, self.half)
        src = self.x.at[pl.ds(self.spot[rel] + shift, size)]
        dst = src if slot is None else self.buf.at[pl.ds(self.buf_at + slot * self.n + shift, size)]
        return remote(src, dst, self.sems, self.sem_at + m, self.peers[way])

    def start(self, which):
        for m in which:
            self.copy(m).start()

    def take(self, which):
        for m in which:
            self.copy(m).wait_recv()

    def sent(self, which):
        for m in which:
            self.copy(m).wait_send()

    def rs_pass(self):
        self.take(FAR[:1])
        add_into(self.x, self.spot[RIGHT], [(self.buf, self.buf_at)], self.half)
        self.start(ON[:1])
        self.take(FAR[1:])
        add_into(self.x, self.spot[LEFT] + self.half, [(self.buf, self.buf_at + self.half)], self.rest)
        self.start(ON[1:])

    def rs_end(self):
        self.take(NEAR + ON)
        got = [(self.buf, self.buf_at + slot * self.n) for slot in (1, 2)]
        add_into(self.x, self.spot[OWN], got, self.n)

    def ag_pass(self):
        for first, then in zip(GATHER[:2], GATHER[4:]):
            self.copy(first).wait_recv()
            self.copy(then).start()


def tower_forward(rows, w_one, w_two, w_proj, ready):
    hidden = rows
    for layer in range(2):
        ready(2 * layer)
        act = jax.nn.gelu(dot(hidden, w_one[layer])).astype(BF16)
        ready(2 * layer + 1)
        hidden = (hidden.astype(F32) + dot(act, w_two[layer])).astype(BF16)
    ready(4)
    return dot(hidden, w_proj[...]).astype(BF16)


def weight_loads(src, dst, sems, at=0):
    pairs = [(one.at[layer], two.at[layer]) for layer in range(2) for one, two in zip(src[:2], dst[:2])]
    return [pltpu.make_async_copy(one, two, sems.at[at + i]) for i, (one, two) in enumerate(pairs + [(src[2], dst[2])])]


def score_kernel(
    tau_ref, q_ref, d_ref, q_w1, q_w2, q_proj, d_w1, d_w2, d_proj, q_up, d_up, loss_ref,
    q_all, d_all, st, stats, q_part, d_part, q_buf, d_buf, pair, loss_all, q_one, q_two, q_last, d_one, d_two, d_last, w_sems, *sems
):
    q_weights, d_weights = (q_one, q_two, q_last), (d_one, d_two, d_last)
    q_loads = weight_loads((q_w1, q_w2, q_proj), q_weights, w_sems)
    d_loads = weight_loads((d_w1, d_w2, d_proj), d_weights, w_sems, len(q_loads))
    for c in q_loads + d_loads:
        c.start()
    at = place()
    core, z = at['core'], at['z']
    other = moved(at, 'core', 1)
    q_peers = [moved(moved(at, 'x', s % SIDE), 'y', s // SIDE) for s in range(1, 16)]
    d_peers = [moved(moved(at, 'core', s % 2), 'z', s // 2) for s in range(1, 8)]
    q_slot, d_slot = at['y'] * SIDE + at['x'], core * SIDE + z
    greet(q_peers + d_peers)

    outer, inner = ('y', 'x'), ('x', 'y')
    own = [at[outer[h]] * 8 + at[inner[h]] * 2 for h in range(2)]

    def q_rings(x, h):
        wide = Ring(at, outer[h], x.at[h], 0, 8, q_buf.at[h], 0, sems, h)
        return wide, Ring(at, inner[h], x.at[h], at[outer[h]] * 8, 2, q_buf.at[h], 24, sems, 2 + h)

    q_wide, q_thin = zip(*[q_rings(q_all, h) for h in range(2)])
    docs_ring = Ring(at, 'z', d_all.at[core], 0, 8, d_buf, 0, sems, 4)
    hands_at = 5 * len(MESSAGES)
    def hand(rel):
        here = d_all.at[core, pl.ds(docs_ring.spot[rel], 8)]
        return remote(here, here, sems, hands_at + rel, other)

    for h in range(2):
        def q_body(i, carry):
            def ready(step):
                if h == 0:
                    pl.when(i == 0)(q_loads[step].wait)

            rows = pl.ds(pl.multiple_of((h * 2 + i) * 16, 16), 16)
            q_all[h, own[h] + i] = tower_forward(q_ref[rows, :], *q_weights, ready)
            return carry

        lax.fori_loop(0, 2, q_body, 0)
        if h == 0:
            pl.semaphore_wait(pltpu.get_barrier_semaphore(), len(q_peers) + len(d_peers))
        q_thin[h].start(FIRST + SECOND)
    for c in d_loads:
        c.wait()

    def d_body(i, carry):
        rows = pl.ds(pl.multiple_of(i * 32, 32), 32)
        d_all[core, pl.ds(z * 8 + i * 2, 2)] = tower_forward(d_ref[rows, :], *d_weights, lambda step: None).reshape(2, 16, DIM)

        @pl.when(i == 0)
        def _():
            for ring in q_thin:
                ring.ag_pass()

        @pl.when(i == 1)
        def _():
            docs_ring.start(FIRST[:1] + SECOND[1:])
            for thin, wide in zip(q_thin, q_wide):
                thin.take(SECOND + ONWARD)
                wide.start(FIRST + SECOND)

        return carry

    lax.fori_loop(0, SUB_COUNT, d_body, 0)
    docs_ring.start(FIRST[1:] + SECOND[:1])
    hand(OWN).start()
    for ring in q_wide:
        ring.ag_pass()
    docs_ring.ag_pass()
    docs_ring.take(SECOND)
    hand(LEFT).start()
    hand(RIGHT).start()
    docs_ring.take(ONWARD)
    hand(ACROSS).start()
    for ring in q_wide:
        ring.take(SECOND + ONWARD)
    for rel in range(SIDE):
        hand(rel).wait_recv()

    tau = tau_ref[0]
    queries = q_all[...].reshape(1024, DIM)
    blocks = [(c, j) for c in range(2) for j in range(SIDE)]

    def block(ref, c, j):
        return ref[c, j * 8:(j + 1) * 8].reshape(128, DIM)

    highs = []
    for b, (c, j) in enumerate(blocks):
        tile = dot(block(d_all, c, j), queries, LAST_CONTRACT) / tau
        st[b] = tile
        highs.append(jnp.max(tile, axis=0, keepdims=True))
    high = functools.reduce(jnp.maximum, highs)
    total = sum(jnp.sum(jnp.exp(st[b] - high), axis=0, keepdims=True) for b in range(len(blocks)))

    def matches(rows):
        row = lax.broadcasted_iota(jnp.int32, (rows, 1024), 0)
        column = lax.broadcasted_iota(jnp.int32, (rows, 1024), 1)
        return (row < 64) & (column == jnp.where(row < 32, own[0] * 16 + row, 480 + own[1] * 16 + row))

    positive = jnp.sum(jnp.where(matches(64), st[d_slot, 0:64, :], 0.0), axis=0, keepdims=True)
    for i, row in enumerate((high, total, positive)):
        stats[q_slot, i:i + 1, :] = row
    extra = hands_at + SIDE
    shares = [remote(stats.at[q_slot], stats.at[q_slot], sems, extra + i, p) for i, p in enumerate(q_peers)]
    for c in shares:
        c.start()
    for c in shares:
        c.wait_recv()
    all_stats = [stats[j] for j in range(16)]
    top = functools.reduce(jnp.maximum, [s[0:1] for s in all_stats])
    norm = sum(s[1:2] * jnp.exp(s[0:1] - top) for s in all_stats)
    log_norm = top + jnp.log(norm)
    part = jnp.sum(log_norm - sum(s[2:3] for s in all_stats), axis=1, keepdims=True)
    loss_all[d_slot] = jnp.broadcast_to(part, (8, 128))
    extra = extra + len(shares)
    losses = [remote(loss_all.at[d_slot], loss_all.at[d_slot], sems, extra + i, p) for i, p in enumerate(d_peers)]
    for c in losses:
        c.start()

    scale = 8192.0 * tau
    hit = matches(128)
    grads = []
    for b in range(len(blocks)):
        soft = jnp.exp(st[b] - log_norm) - jnp.where(hit & (d_slot == b), 1.0, 0.0)
        grads.append((soft / scale).astype(BF16))
    grad = jnp.concatenate(grads, axis=0)
    docs = d_all[...].reshape(1024, DIM)
    q_wide, q_thin = zip(*[q_rings(q_part, h) for h in range(2)])
    for h in range(2):
        q_part[h] = dot(grad[:, h * DIM:(h + 1) * DIM], docs, ROWS_CONTRACT).reshape(32, 16, DIM)
        q_wide[h].start(FAR + NEAR)

    extra = extra + len(losses)
    for b, (c, j) in enumerate(blocks):
        d_part[c, j * 8:(j + 1) * 8] = dot(grads[b], queries).reshape(8, 16, DIM)
    swap = remote(d_part.at[other['core']], pair, sems, extra, other)
    swap.start()
    docs_sum = Ring(at, 'z', d_part.at[core], 0, 8, d_buf, 0, sems, 4)
    q_wide[0].rs_pass()
    swap.wait_recv()
    add_into(d_part.at[core], 0, [(pair, 0)], 32)
    docs_sum.start(FAR + NEAR)
    q_wide[1].rs_pass()
    for wide, thin in zip(q_wide, q_thin):
        wide.rs_end()
        thin.start(FAR + NEAR)
    docs_sum.rs_pass()
    for ring in q_thin:
        ring.rs_pass()
    for c in losses:
        c.wait_recv()
    loss_ref[...] = sum(loss_all[j, 0:1, 0:1] for j in range(8)) / 8192.0
    for h, ring in enumerate(q_thin):
        ring.rs_end()
        q_up[h * 32:(h + 1) * 32, :] = q_part[h, pl.ds(own[h], 2)].reshape(32, DIM).astype(BF16)
    docs_sum.rs_end()
    d_up[...] = d_part[core, pl.ds(z * 8, 8)].reshape(128, DIM).astype(BF16)
    for c in shares + losses + [swap] + list(map(hand, range(SIDE))):
        c.wait_send()
    for ring in (*q_wide, *q_thin, docs_sum):
        ring.sent(FAR + NEAR + ON)
    for h in range(2):
        for ring in q_rings(q_all, h):
            ring.sent(GATHER)
    docs_ring.sent(GATHER)


def scores(tau, q_rows, d_rows, weights):
    vmem, whole = pl.BlockSpec(memory_space=pltpu.VMEM), pl.BlockSpec(memory_space=pl.ANY)
    copies = 5 * len(MESSAGES) + 27
    return pl.pallas_call(
        score_kernel,
        out_shape=tuple(jax.ShapeDtypeStruct(*s) for s in (((64, DIM), BF16), ((128, DIM), BF16), ((1, 1), F32))),
        in_specs=[pl.BlockSpec(memory_space=pltpu.SMEM), vmem, vmem] + [whole] * 6,
        out_specs=(vmem,) * 3,
        scratch_shapes=[
            pltpu.VMEM((2, 32, 16, DIM), BF16),
            pltpu.VMEM((2, 32, 16, DIM), BF16),
            pltpu.VMEM((8, 128, 1024), F32),
            pltpu.VMEM((16, 3, 1024), F32),
            pltpu.VMEM((2, 32, 16, DIM), F32),
            pltpu.VMEM((2, 32, 16, DIM), F32),
            pltpu.VMEM((2, 30, 16, DIM), F32),
            pltpu.VMEM((24, 16, DIM), F32),
            pltpu.VMEM((32, 16, DIM), F32),
            pltpu.VMEM((8, 8, 128), F32),
            *[pltpu.VMEM(shape, BF16) for shape in WEIGHT_SHAPES * 2],
            pltpu.SemaphoreType.DMA((10,)),
            pltpu.SemaphoreType.DMA((copies,)),
            pltpu.SemaphoreType.DMA((copies,)),
        ],
        compiler_params=pltpu.CompilerParams(collective_id=0, has_side_effects=True, vmem_limit_bytes=VMEM_LIMIT),
        name='towers_forward_scores',
    )(tau, q_rows, d_rows, *weights)


def gelu_back(pre, act_grad):
    return jax.vjp(jax.nn.gelu, pre)[1](act_grad)[0]


def tower_backward(sub, rows_per, x_ref, up_ref, w_one, w_two, w_proj, acc, pre_s, act_s, hook):
    rows = pl.ds(pl.multiple_of(sub * rows_per, rows_per), rows_per)
    hidden = [x_ref[rows, :]]
    for layer in range(2):
        pre = dot(hidden[layer], w_one[layer])
        pre_s[layer, 0:rows_per] = pre
        act = jax.nn.gelu(pre).astype(BF16)
        act_s[layer, 0:rows_per] = act
        if layer == 0:
            hook(0)
        hidden.append((hidden[layer].astype(F32) + dot(act, w_two[layer])).astype(BF16))
    hook(1)
    up = up_ref[rows, :]

    def add(base, stride, lhs, rhs):
        for i in range(lhs.shape[1] // COLS):
            part = dot(lhs[:, i * COLS:(i + 1) * COLS], rhs, ROWS_CONTRACT)
            for j in range(2):
                spot = base + j * stride + i * 32
                acc[spot:spot + 32] += part[:, j * COLS:(j + 1) * COLS].reshape(32, 8, COLS)

    add(FFN, 64, hidden[2], up)
    resid = dot(up, w_proj[...], LAST_CONTRACT)
    for layer in (1, 0):
        resid_bf = resid.astype(BF16)
        add(1024 + layer * DIM, COLS, act_s[layer, 0:rows_per], resid_bf)
        act_grad = dot(resid_bf, w_two[layer], LAST_CONTRACT)
        pre_grad = gelu_back(pre_s[layer, 0:rows_per], act_grad).astype(BF16)
        for c in range(4):
            add(layer * DIM + c * 128, 64, hidden[layer], pre_grad[:, c * DIM:(c + 1) * DIM])
        if layer == 1:
            resid = resid + dot(pre_grad, w_one[layer], LAST_CONTRACT)
            hook(2)
    hook(3)


class Exchange:
    def __init__(self, acc, pair, bufs, sems):
        self.acc, self.pair = acc, pair
        self.pair_sems, self.ring_sems, self.hand_sems, self.credit, self.ready = sems[:2], sems[2:4], sems[4:6], sems[6], sems[7]
        self.at = place()
        self.core = self.at['core']
        self.other = moved(self.at, 'core', 1)
        self.around = [moved(self.at, d, s) for d in 'xyz' for s in (LEFT, RIGHT)]
        greet([self.other] + self.around)
        self.rings = {}
        for t in (Q, D):
            for k, (first, rows, dims) in enumerate(COLOURS):
                base = self.core * HALF + first
                for p in (OUTER, MIDDLE, INNER):
                    n = rows * RING_SIZE[p]
                    index = (t * len(COLOURS) + k) * len(RING_SIZE) + p
                    self.rings[t, k, p] = Ring(self.at, dims[p], acc.at[t], base, n, bufs[p], 3 * first // SIDE ** (p + 1), self.ring_sems, index)
                    base = base + self.at[dims[p]] * n

    def met(self):
        pl.semaphore_wait(pltpu.get_barrier_semaphore(), len(self.around) + 1)

    def level(self, t, p):
        return [self.rings[t, k, p] for k in range(len(COLOURS))]

    def pair_copy(self, t, rel, k):
        first, ring = COLOURS[k][0], self.rings[t, k, OUTER]
        spot = ring.spot[rel] + (1 - self.core * 2) * HALF
        dst = self.pair.at[PAIR_SLOT[rel], pl.ds(first // SIDE, ring.n)]
        return remote(self.acc.at[t, pl.ds(spot, ring.n)], dst, self.pair_sems, t * 12 + rel * 3 + k, self.other)

    def pairs(self, t, rel, fresh=False):
        if not fresh:
            pl.semaphore_wait(self.credit.at[PAIR_SLOT[rel]], 1)
        for k in range(len(COLOURS)):
            self.pair_copy(t, rel, k).start()

    def settle(self, t, rel, last=False):
        for k, ring in enumerate(self.level(t, OUTER)):
            self.pair_copy(t, rel, k).wait_recv()
            add_into(ring.x, ring.spot[rel], [(self.pair.at[PAIR_SLOT[rel]], COLOURS[k][0] // SIDE)], ring.n)
        if not last:
            pl.semaphore_signal(self.credit.at[PAIR_SLOT[rel]], inc=1, device_id=device(self.other), device_id_type=MESH)

    def start(self, t, p, which):
        for ring in self.level(t, p):
            ring.start(which)

    def rs_pass(self, t, p):
        for ring in self.level(t, p):
            ring.rs_pass()

    def rs_end(self, t, p):
        for ring in self.level(t, p):
            ring.rs_end()
        for k, ring in enumerate(self.level(t, p)):
            ring.sent(FAR + NEAR + ON)
            for rel in range(SIDE) if p == OUTER else ():
                self.pair_copy(t, rel, k).wait_send()
        for peer in self.around:
            pl.semaphore_signal(self.ready.at[t * 3 + p], inc=1, device_id=device(peer), device_id_type=MESH)
        if p == OUTER:
            pl.semaphore_signal(self.ready.at[6 + t], inc=1, device_id=device(self.other), device_id_type=MESH)

    def opened(self, t, p):
        pl.semaphore_wait(self.ready.at[t * 3 + p], len(self.around))

    def hand(self, t, k, p, rel, second):
        ring = self.rings[t, k, p]
        shift, size = (0, ring.n) if rel != ACROSS else (ring.half, ring.rest) if second else (0, ring.half)
        here = self.acc.at[t, pl.ds(ring.spot[rel] + shift, size)]
        kind = HANDS.index((rel, second))
        return remote(here, here, self.hand_sems, ((t * 3 + k) * 3 + p) * len(HANDS) + kind, self.other)

    def ag_start(self, t, p, which=FIRST + SECOND):
        self.start(t, p, which)
        if p == INNER:
            pl.semaphore_wait(self.ready.at[6 + t], 1)
            for k in range(len(COLOURS)):
                self.hand(t, k, p, OWN, False).start()

    def ag_pass(self, t, p):
        for ring in self.level(t, p):
            ring.ag_pass()
        for k, ring in enumerate(self.level(t, p)):
            for m, rel in zip(SECOND, (LEFT, RIGHT)):
                ring.take((m,))
                self.hand(t, k, p, rel, False).start()

    def ag_end(self, t, p):
        for k, ring in enumerate(self.level(t, p)):
            for m, second in zip(ONWARD, (False, True)):
                ring.take((m,))
                self.hand(t, k, p, ACROSS, second).start()

    def finish(self):
        hands = [(t, k, p, *h) for t, k, p in self.rings for h in HANDS if h[0] != OWN or p == INNER]
        for h in hands:
            self.hand(*h).wait_recv()
        for ring in self.rings.values():
            ring.sent(GATHER)
        for h in hands:
            self.hand(*h).wait_send()


def train_kernel(q_in, d_in, q_up, d_up, q_w1, q_w2, q_proj, d_w1, d_w2, d_proj, acc, w_one, w_two, w_proj, pre_s, act_s, pair, *rest):
    bufs, w_sems, sems = rest[:3], rest[3], rest[4:]
    ex = Exchange(acc, pair, bufs, sems)

    held = (w_one, w_two, w_proj)
    q_loads, d_loads = weight_loads((q_w1, q_w2, q_proj), held, w_sems), weight_loads((d_w1, d_w2, d_proj), held, w_sems)
    for c in q_loads:
        c.start()

    def clear(i, carry):
        for t in (Q, D):
            acc[t, pl.ds(i * 16, 16)] = jnp.zeros((16, 8, COLS), F32)
        return carry

    lax.fori_loop(0, UNITS // 16, clear, 0)
    for c in q_loads:
        c.wait()

    def at_hooks(sub, table):
        def hook(i):
            for when, work in table:
                if when[1] == i:
                    pl.when(sub == when[0])(work)

        return hook

    def swap_early():
        d_loads[0].start()

    def swap_late():
        for c in d_loads[2:]:
            c.start()

    def q_body(sub, carry):
        hook = at_hooks(sub, (((3, 1), swap_early), ((3, 2), swap_late)))
        tower_backward(sub, 16, q_in, q_up, *held, acc.at[Q], pre_s, act_s, hook)
        return carry

    lax.fori_loop(0, SUB_COUNT, q_body, 0)
    d_loads[1].start()
    ex.met()
    ex.pairs(Q, ACROSS, fresh=True)
    ex.pairs(Q, RIGHT, fresh=True)
    d_loads[0].wait()
    for c in d_loads[2:]:
        c.wait()

    def across():
        ex.settle(Q, ACROSS)
        ex.start(Q, OUTER, FAR)

    def right():
        ex.pairs(Q, LEFT)
        ex.settle(Q, RIGHT)

    def left():
        ex.settle(Q, LEFT)
        ex.start(Q, OUTER, NEAR)

    def own():
        ex.settle(Q, OWN)
        ex.rs_pass(Q, OUTER)

    steps = (
        ((0, 0), d_loads[1].wait), ((0, 2), across), ((0, 3), right),
        ((1, 1), functools.partial(ex.pairs, Q, OWN)), ((1, 2), left), ((1, 3), own),
    )

    def d_body(sub, carry):
        tower_backward(sub, 32, d_in, d_up, *held, acc.at[D], pre_s, act_s, at_hooks(sub, steps))
        return carry

    lax.fori_loop(0, SUB_COUNT, d_body, 0)
    ex.pairs(D, ACROSS)
    ex.pairs(D, RIGHT)
    ex.rs_end(Q, OUTER)
    ex.start(Q, MIDDLE, FAR + NEAR)
    ex.settle(D, ACROSS)
    ex.pairs(D, LEFT)
    ex.rs_pass(Q, MIDDLE)
    ex.opened(Q, OUTER)
    ex.start(D, OUTER, FAR)
    ex.settle(D, RIGHT)
    ex.pairs(D, OWN)
    ex.rs_end(Q, MIDDLE)
    ex.start(Q, INNER, FAR + NEAR)
    ex.settle(D, LEFT, last=True)
    ex.start(D, OUTER, NEAR)
    ex.settle(D, OWN, last=True)
    ex.rs_pass(Q, INNER)
    ex.rs_pass(D, OUTER)
    ex.rs_end(Q, INNER)
    ex.opened(Q, INNER)
    ex.ag_start(Q, INNER)
    ex.rs_end(D, OUTER)
    ex.opened(Q, MIDDLE)
    ex.start(D, MIDDLE, FAR + NEAR)
    ex.ag_pass(Q, INNER)
    ex.ag_end(Q, INNER)
    ex.ag_start(Q, MIDDLE)
    ex.rs_pass(D, MIDDLE)
    ex.ag_pass(Q, MIDDLE)
    ex.rs_end(D, MIDDLE)
    ex.start(D, INNER, FAR + NEAR)
    ex.ag_end(Q, MIDDLE)
    ex.ag_start(Q, OUTER, FIRST)
    ex.rs_pass(D, INNER)
    ex.rs_end(D, INNER)
    ex.opened(D, INNER)
    ex.ag_start(D, INNER)
    ex.ag_start(Q, OUTER, SECOND)
    ex.ag_pass(D, INNER)
    ex.ag_pass(Q, OUTER)
    ex.ag_end(D, INNER)
    ex.opened(D, MIDDLE)
    ex.ag_start(D, MIDDLE)
    ex.ag_pass(D, MIDDLE)
    ex.ag_end(Q, OUTER)
    ex.ag_end(D, MIDDLE)
    ex.opened(D, OUTER)
    ex.ag_start(D, OUTER)
    ex.ag_pass(D, OUTER)
    ex.ag_end(D, OUTER)
    ex.finish()


def train(q_rows, d_rows, q_up, d_up, weights):
    vmem, whole = pl.BlockSpec(memory_space=pltpu.VMEM), pl.BlockSpec(memory_space=pl.ANY)
    bufs = [pltpu.VMEM((3 * HALF // SIDE ** p // SIDE, 8, COLS), F32) for p in (OUTER, MIDDLE, INNER)]
    dma = pltpu.SemaphoreType.DMA
    return pl.pallas_call(
        train_kernel,
        out_shape=pltpu.VMEM((2, UNITS, 8, COLS), F32),
        in_specs=[vmem] * 4 + [whole] * 6,
        out_specs=vmem,
        scratch_shapes=[
            *[pltpu.VMEM(shape, BF16) for shape in WEIGHT_SHAPES],
            pltpu.VMEM((2, 32, FFN), F32),
            pltpu.VMEM((2, 32, FFN), BF16),
            pltpu.VMEM((2, 272, 8, COLS), F32),
            *bufs,
            dma((5,)), *[dma((n,)) for n in (24, 24, 216, 216, 90, 90)],
            pltpu.SemaphoreType.REGULAR((2,)), pltpu.SemaphoreType.REGULAR((8,)),
        ],
        compiler_params=pltpu.CompilerParams(collective_id=1, has_side_effects=True, vmem_limit_bytes=TRAIN_VMEM),
        name='towers_backward_all_reduce',
    )(q_rows, d_rows, q_up, d_up, *weights)


def unpack_kernel(acc, *rest):
    outs, sem = rest[:6], rest[6]
    copies = []
    for t in range(2):
        one, two, proj = outs[t * 3:t * 3 + 3]
        for k in range(2):
            for c in range(8):
                copies.append((acc.at[t, pl.ds(k * DIM + c * 64, 64)], one.at[k, :, :, pl.ds(c * COLS, COLS)]))
            for c in range(2):
                copies.append((acc.at[t, pl.ds(1024 + k * DIM + c * COLS, COLS)], two.at[k, :, :, pl.ds(c * COLS, COLS)]))
        for c in range(2):
            copies.append((acc.at[t, pl.ds(FFN + c * 64, 64)], proj.at[:, :, pl.ds(c * COLS, COLS)]))
    copies = [pltpu.make_async_copy(src, dst, sem.at[i]) for i, (src, dst) in enumerate(copies)]
    for c in copies:
        c.start()
    for c in copies:
        c.wait()


def unpack(acc):
    shapes = ((2, 64, 8, FFN), (2, COLS, 8, DIM), (64, 8, DIM)) * 2
    outs = pl.pallas_call(
        unpack_kernel,
        out_shape=tuple(jax.ShapeDtypeStruct(s, F32) for s in shapes),
        in_specs=[pl.BlockSpec(memory_space=pltpu.VMEM)],
        out_specs=(pl.BlockSpec(memory_space=pl.ANY),) * 6,
        scratch_shapes=[pltpu.SemaphoreType.DMA((44,))],
        compiler_params=pltpu.CompilerParams(vmem_limit_bytes=1 << 20),
        name='unpack',
    )(acc)
    return tuple(o.reshape(s) for o, s in zip(outs, WEIGHT_SHAPES * 2))


def local_step(q_loc, d_loc, temperature, *weights):
    d_rows = d_loc.reshape(-1, d_loc.shape[-1])
    q_up, d_up, loss = scores(temperature.reshape(1), q_loc, d_rows, weights)
    return (loss.reshape(()), *unpack(train(q_loc, d_rows, q_up, d_up, weights)))


def solution(mesh):
    specs_in = (P('data', None), P(None, 'data', None), P(), P(), P(), P(), P(), P(), P())
    specs_out = (P(), P(), P(), P(), P(), P(), P())
    return jax.shard_map(local_step, mesh=mesh, in_specs=specs_in, out_specs=specs_out, check_vma=False)
```

```python
import functools

import jax
import jax.numpy as jnp
from jax import lax
from jax.experimental import pallas as pl
from jax.experimental.pallas import tpu as pltpu
from jax.sharding import PartitionSpec as P

F32 = jnp.float32
BF16 = jnp.bfloat16
MESH = pl.DeviceIdType.MESH
SUB_COUNT = 4
SIDE = 4
ROWS_CONTRACT = (((0,), (0,)), ((), ()))
LAST_CONTRACT = (((1,), (1,)), ((), ()))
SCORE_VMEM = 67043328

UNITS = 2176
HALF = 1088
TRAIN_VMEM = 27500000
PAIR_SLOT = (1, 1, 0, 0)
RING_SIZE = (16, 4, 1)
Q, D = range(2)
OUTER, MIDDLE, INNER = range(3)
OWN, RIGHT, ACROSS, LEFT = range(4)
MESSAGES = (
    (ACROSS, False, 0, 0), (ACROSS, True, 1, 0), (RIGHT, True, 0, 1), (LEFT, False, 1, 2), (RIGHT, False, 0, 1), (LEFT, True, 1, 2),
    (OWN, False, 0, None), (OWN, True, 1, None), (OWN, True, 0, None), (OWN, False, 1, None), (LEFT, False, 0, None), (RIGHT, True, 1, None),
)
ALL = tuple(range(len(MESSAGES)))
FAR, NEAR, ON, GATHER = ALL[:2], ALL[2:4], ALL[4:6], ALL[6:]
FIRST, SECOND, ONWARD = GATHER[:2], GATHER[2:4], GATHER[4:]
DIM, FFN, COLS = 512, 2048, 256
WEIGHT_SHAPES = ((2, DIM, FFN), (2, FFN, DIM), (DIM, DIM))
COLOURS = ((0, 6), (384, 6), (768, 5))
ORDERS = (('xyz', 'yzx', 'zxy'), ('zxy', 'xyz', 'yzx'))
HANDS = ((LEFT, False), (RIGHT, False), (ACROSS, False), (ACROSS, True), (OWN, False))


def place():
    me = lax.axis_index('data')
    core = lax.rem(me, 2)
    x = lax.rem(me // 2, SIDE)
    y = lax.rem(me // 8, SIDE)
    z = me // 32
    return dict(z=z, y=y, x=x, core=core)


def device(at):
    return (((at['z'] * SIDE + at['y']) * SIDE + at['x']) * 2 + at['core'],)


def moved(at, dim, step):
    size = 2 if dim == 'core' else SIDE
    return {**at, dim: lax.rem(at[dim] + step, size)}


def remote(src, dst, sems, index, peer):
    return pltpu.make_async_remote_copy(
        src_ref=src, dst_ref=dst, send_sem=sems[0].at[index], recv_sem=sems[1].at[index], device_id=device(peer), device_id_type=MESH
    )


def greet(peers):
    for peer in peers:
        pl.semaphore_signal(pltpu.get_barrier_semaphore(), inc=1, device_id=device(peer), device_id_type=MESH)


def dot(lhs, rhs, dims=None):
    if dims is None:
        return jnp.dot(lhs, rhs, preferred_element_type=F32)
    return lax.dot_general(lhs, rhs, dims, preferred_element_type=F32)


def add_into(dst, dst_at, pieces, size):
    step = next(s for s in (16, 12, 10, 8, 6, 5, 4, 3, 2, 1) if size % s == 0)

    def body(i, carry):
        here = pl.ds(dst_at + i * step, step)
        total = dst[here]
        for ref, ref_at in pieces:
            total = total + ref[pl.ds(ref_at + i * step, step)]
        dst[here] = total
        return carry

    lax.fori_loop(0, size // step, body, 0)


class Ring:
    def __init__(self, at, dim, x, base, n, buf, buf_at, sems, sem_at):
        self.x, self.n, self.buf, self.buf_at = x, n, buf, buf_at
        self.half = (n + 1) // 2
        self.rest = n - self.half
        self.spot = [base + lax.rem(at[dim] + rel, SIDE) * n for rel in range(SIDE)]
        self.peers = moved(at, dim, RIGHT), moved(at, dim, LEFT)
        self.sems, self.sem_at = sems, sem_at * len(MESSAGES)

    def copy(self, m):
        rel, second, way, slot = MESSAGES[m]
        shift, size = (self.half, self.rest) if second else (0, self.half)
        src = self.x.at[pl.ds(self.spot[rel] + shift, size)]
        dst = src if slot is None else self.buf.at[pl.ds(self.buf_at + slot * self.n + shift, size)]
        return remote(src, dst, self.sems, self.sem_at + m, self.peers[way])

    def start(self, which):
        for m in which:
            self.copy(m).start()

    def take(self, which):
        for m in which:
            self.copy(m).wait_recv()

    def sent(self, which):
        for m in which:
            self.copy(m).wait_send()

    def rs_pass(self):
        self.take(FAR[:1])
        add_into(self.x, self.spot[RIGHT], [(self.buf, self.buf_at)], self.half)
        self.start(ON[:1])
        self.take(FAR[1:])
        add_into(self.x, self.spot[LEFT] + self.half, [(self.buf, self.buf_at + self.half)], self.rest)
        self.start(ON[1:])

    def rs_end(self):
        self.take(NEAR + ON)
        got = [(self.buf, self.buf_at + slot * self.n) for slot in (1, 2)]
        add_into(self.x, self.spot[OWN], got, self.n)

    def ag_pass(self):
        for first, then in zip(GATHER[:2], GATHER[4:]):
            self.copy(first).wait_recv()
            self.copy(then).start()


def tower_forward(rows, w_one, w_two, w_proj, ready):
    hidden = rows
    for layer in range(2):
        ready(2 * layer)
        act = jax.nn.gelu(dot(hidden, w_one[layer])).astype(BF16)
        ready(2 * layer + 1)
        hidden = (hidden.astype(F32) + dot(act, w_two[layer])).astype(BF16)
    ready(4)
    return dot(hidden, w_proj[...]).astype(BF16)


def up_rows(ups):
    return ups.at[pl.ds(0, 64)], ups.at[pl.ds(64, 128)]


def arrivals(pairs, sems):
    copies = [pltpu.make_async_copy(src, dst, sems.at[i]) for i, (src, dst) in enumerate(pairs)]
    for c in copies:
        c.start()
    return copies


def weight_loads(src, dst, sems, at=0):
    pairs = [(one.at[layer], two.at[layer]) for layer in range(2) for one, two in zip(src[:2], dst[:2])]
    return [pltpu.make_async_copy(one, two, sems.at[at + i]) for i, (one, two) in enumerate(pairs + [(src[2], dst[2])])]


def score_kernel(
    tau_ref, q_ref, d_ref, q_w1, q_w2, q_proj, d_w1, d_w2, d_proj, ups, loss_ref,
    q_all, d_all, st, stats, q_part, d_part, q_buf, d_buf, pair, loss_all, loss_row, q_one, q_two, q_last, d_one, d_two, d_last, w_sems, *sems
):
    q_weights, d_weights = (q_one, q_two, q_last), (d_one, d_two, d_last)
    q_loads = weight_loads((q_w1, q_w2, q_proj), q_weights, w_sems)
    d_loads = weight_loads((d_w1, d_w2, d_proj), d_weights, w_sems, len(q_loads))
    for c in q_loads + d_loads:
        c.start()
    q_up, d_up = up_rows(ups)
    at = place()
    core, z = at['core'], at['z']
    other = moved(at, 'core', 1)
    q_peers = [moved(moved(at, 'x', s % SIDE), 'y', s // SIDE) for s in range(1, 16)]
    d_peers = [moved(moved(at, 'core', s % 2), 'z', s // 2) for s in range(1, 8)]
    q_slot, d_slot = at['y'] * SIDE + at['x'], core * SIDE + z
    greet(q_peers + d_peers)

    outer, inner = ('y', 'x'), ('x', 'y')
    own = [at[outer[h]] * 8 + at[inner[h]] * 2 for h in range(2)]

    def q_rings(x, h):
        wide = Ring(at, outer[h], x.at[h], 0, 8, q_buf.at[h], 0, sems, h)
        return wide, Ring(at, inner[h], x.at[h], at[outer[h]] * 8, 2, q_buf.at[h], 24, sems, 2 + h)

    q_wide, q_thin = zip(*[q_rings(q_all, h) for h in range(2)])
    docs_ring = Ring(at, 'z', d_all.at[core], 0, 8, d_buf, 0, sems, 4)
    hands_at = 5 * len(MESSAGES)
    def hand(rel):
        here = d_all.at[core, pl.ds(docs_ring.spot[rel], 8)]
        return remote(here, here, sems, hands_at + rel, other)

    used = [hands_at + SIDE + 1]

    def broadcast(src, peers):
        copies = [remote(src, src, sems, used[0] + i, p) for i, p in enumerate(peers)]
        used[0] += len(peers)
        for c in copies:
            c.start()
        return copies

    for h in range(2):
        def q_body(i, carry):
            def ready(step):
                if h == 0:
                    pl.when(i == 0)(q_loads[step].wait)

            rows = pl.ds(pl.multiple_of((h * 2 + i) * 16, 16), 16)
            q_all[h, own[h] + i] = tower_forward(q_ref[rows, :], *q_weights, ready)
            return carry

        lax.fori_loop(0, 2, q_body, 0)
        if h == 0:
            pl.semaphore_wait(pltpu.get_barrier_semaphore(), len(q_peers) + len(d_peers))
        q_thin[h].start(FIRST + SECOND)
    for c in d_loads:
        c.wait()

    def d_body(i, carry):
        rows = pl.ds(pl.multiple_of(i * 32, 32), 32)
        d_all[core, pl.ds(z * 8 + i * 2, 2)] = tower_forward(d_ref[rows, :], *d_weights, lambda step: None).reshape(2, 16, DIM)

        @pl.when(i == 1)
        def _():
            docs_ring.start(FIRST[:1] + SECOND[1:])
            for ring in q_thin:
                ring.ag_pass()

        @pl.when(i == 2)
        def _():
            for thin, wide in zip(q_thin, q_wide):
                thin.take(SECOND + ONWARD)
                wide.start(FIRST + SECOND)

        return carry

    lax.fori_loop(0, SUB_COUNT, d_body, 0)
    docs_ring.start(FIRST[1:] + SECOND[:1])
    hand(OWN).start()
    docs_ring.take(FIRST[:1])
    docs_ring.start(ONWARD[:1])
    for ring in q_wide:
        ring.ag_pass()
    docs_ring.take(FIRST[1:])
    docs_ring.start(ONWARD[1:])
    docs_ring.take(SECOND)
    hand(LEFT).start()
    hand(RIGHT).start()
    docs_ring.take(ONWARD)
    hand(ACROSS).start()
    for ring in q_wide:
        ring.take(SECOND + ONWARD)
    for rel in range(SIDE):
        hand(rel).wait_recv()

    tau = tau_ref[0]
    queries = q_all[...].reshape(1024, DIM)
    docs = d_all[...].reshape(1024, DIM)
    highs = []
    for b in range(SIDE):
        rows = slice(b * COLS, (b + 1) * COLS)
        tile = dot(docs[rows], queries, LAST_CONTRACT) / tau
        st[rows] = tile
        highs.append(jnp.max(tile, axis=0, keepdims=True))
    high = functools.reduce(jnp.maximum, highs)
    blocks = [slice(b * 128, (b + 1) * 128) for b in range(8)]
    total = sum(jnp.sum(jnp.exp(st[rows] - high), axis=0, keepdims=True) for rows in blocks)
    stats[q_slot] = high + jnp.log(total)
    shares = broadcast(stats.at[q_slot], q_peers)
    for c in shares:
        c.wait_recv()
    all_stats = [stats[j] for j in range(16)]
    top = functools.reduce(jnp.maximum, all_stats)
    log_norm = top + jnp.log(sum(jnp.exp(part - top) for part in all_stats))

    def matches(rows):
        row = lax.broadcasted_iota(jnp.int32, (rows, 1024), 0)
        column = lax.broadcasted_iota(jnp.int32, (rows, 1024), 1)
        return (row < 64) & (column == jnp.where(row < 32, own[0] * 16 + row, 480 + own[1] * 16 + row))

    def spread(values):
        return jnp.broadcast_to(jnp.sum(values, keepdims=True), (1, 128))

    positive = st[pl.ds(pl.multiple_of(d_slot * 128, 128), 64), :]
    loss_all[d_slot] = spread(jnp.where(matches(64), log_norm - positive, 0.0))
    losses = broadcast(loss_all.at[d_slot], d_peers)

    scale = 8192.0 * tau
    hit = matches(128)
    grads = []
    for b, rows in enumerate(blocks):
        soft = jnp.exp(st[rows] - log_norm) - jnp.where(hit & (d_slot == b), 1.0, 0.0)
        grads.append((soft / scale).astype(BF16))
    grad = jnp.concatenate(grads, axis=0)
    q_wide, q_thin = zip(*[q_rings(q_part, h) for h in range(2)])
    for h in range(2):
        q_part[h] = dot(grad[:, h * DIM:(h + 1) * DIM], docs, ROWS_CONTRACT).reshape(32, 16, DIM)
        q_wide[h].start(FAR + NEAR)
    for c in range(2):
        d_part[c] = dot(grad[c * DIM:(c + 1) * DIM], queries).reshape(32, 16, DIM)
    swap = remote(d_part.at[other['core']], pair, sems, hands_at + SIDE, other)
    swap.start()
    docs_sum = Ring(at, 'z', d_part.at[core], 0, 8, d_buf, 0, sems, 4)
    q_wide[0].rs_pass()
    swap.wait_recv()
    add_into(d_part.at[core], 0, [(pair, 0)], 32)
    docs_sum.start(FAR + NEAR)
    q_wide[1].rs_pass()
    for wide, thin in zip(q_wide, q_thin):
        wide.rs_end()
        thin.start(FAR + NEAR)
    docs_sum.rs_pass()
    for c in losses:
        c.wait_recv()
    loss_row[q_slot] = sum(loss_all[j] for j in range(8))
    row_losses = broadcast(loss_row.at[q_slot], q_peers)
    for ring in q_thin:
        ring.rs_pass()
    for h, ring in enumerate(q_thin):
        ring.rs_end()
        q_up[h * 32:(h + 1) * 32, :] = q_part[h, pl.ds(own[h], 2)].reshape(32, DIM).astype(BF16)
    docs_sum.rs_end()
    for c in row_losses:
        c.wait_recv()
    loss_ref[...] = sum(loss_row[j, :, 0:1] for j in range(16)) / 8192.0
    d_up[...] = d_part[core, pl.ds(z * 8, 8)].reshape(128, DIM).astype(BF16)
    for c in shares + losses + row_losses + [swap] + list(map(hand, range(SIDE))):
        c.wait_send()
    for ring in (*q_wide, *q_thin, docs_sum):
        ring.sent(FAR + NEAR + ON)
    for h in range(2):
        for ring in q_rings(q_all, h):
            ring.sent(GATHER)
    docs_ring.sent(GATHER)


def scores(tau, q_rows, d_rows, weights):
    vmem, whole = pl.BlockSpec(memory_space=pltpu.VMEM), pl.BlockSpec(memory_space=pl.ANY)
    copies = 5 * len(MESSAGES) + 42
    return pl.pallas_call(
        score_kernel,
        out_shape=(jax.ShapeDtypeStruct((192, DIM), BF16), jax.ShapeDtypeStruct((1, 1), F32)),
        in_specs=[pl.BlockSpec(memory_space=pltpu.SMEM), vmem, vmem] + [whole] * 6,
        out_specs=(vmem,) * 2,
        scratch_shapes=[
            pltpu.VMEM((2, 32, 16, DIM), BF16),
            pltpu.VMEM((2, 32, 16, DIM), BF16),
            pltpu.VMEM((1024, 1024), F32),
            pltpu.VMEM((16, 1, 1024), F32),
            pltpu.VMEM((2, 32, 16, DIM), F32),
            pltpu.VMEM((2, 32, 16, DIM), F32),
            pltpu.VMEM((2, 30, 16, DIM), F32),
            pltpu.VMEM((24, 16, DIM), F32),
            pltpu.VMEM((32, 16, DIM), F32),
            pltpu.VMEM((8, 1, 128), F32),
            pltpu.VMEM((16, 1, 128), F32),
            *[pltpu.VMEM(shape, BF16) for shape in WEIGHT_SHAPES * 2],
            pltpu.SemaphoreType.DMA((10,)),
            pltpu.SemaphoreType.DMA((copies,)),
            pltpu.SemaphoreType.DMA((copies,)),
        ],
        compiler_params=pltpu.CompilerParams(collective_id=0, has_side_effects=True, vmem_limit_bytes=SCORE_VMEM),
        name='towers_forward_scores',
    )(tau, q_rows, d_rows, *weights)


def gelu_back(pre, act_grad):
    return jax.vjp(jax.nn.gelu, pre)[1](act_grad)[0]


def tower_backward(sub, rows_per, x_ref, up_ref, w_one, w_two, w_proj, acc, pre_s, act_s, hook, ready=None):
    first = ready is not None
    rows = pl.ds(0 if first else pl.multiple_of(sub * rows_per, rows_per), rows_per)
    ready = ready or (lambda step: None)
    hidden = [x_ref[rows, :]]
    for layer in range(2):
        ready(2 * layer)
        pre = dot(hidden[layer], w_one[layer])
        pre_s[layer, 0:rows_per] = pre
        act = jax.nn.gelu(pre).astype(BF16)
        act_s[layer, 0:rows_per] = act
        ready(2 * layer + 1)
        hidden.append((hidden[layer].astype(F32) + dot(act, w_two[layer])).astype(BF16))
    ready(4)
    hook(1)
    up = up_ref[rows, :]

    def add(base, stride, lhs, rhs):
        for i in range(lhs.shape[1] // COLS):
            part = dot(lhs[:, i * COLS:(i + 1) * COLS], rhs, ROWS_CONTRACT)
            for j in range(2):
                spot = base + j * stride + i * 32
                tile = part[:, j * COLS:(j + 1) * COLS].reshape(32, 8, COLS)
                acc[spot:spot + 32] = tile if first else acc[spot:spot + 32] + tile

    add(FFN, 64, hidden[2], up)
    resid = dot(up, w_proj[...], LAST_CONTRACT)
    for layer in (1, 0):
        resid_bf = resid.astype(BF16)
        add(1024 + layer * DIM, COLS, act_s[layer, 0:rows_per], resid_bf)
        act_grad = dot(resid_bf, w_two[layer], LAST_CONTRACT)
        pre_grad = gelu_back(pre_s[layer, 0:rows_per], act_grad).astype(BF16)
        for c in range(4):
            add(layer * DIM + c * 128, 64, hidden[layer], pre_grad[:, c * DIM:(c + 1) * DIM])
        if layer == 1:
            resid = resid + dot(pre_grad, w_one[layer], LAST_CONTRACT)
            hook(2)
    hook(3)


class Exchange:
    def __init__(self, acc, pair, bufs, sems):
        self.acc, self.pair = acc, pair
        self.pair_sems, self.ring_sems, self.hand_sems, self.credit, self.ready = sems[:2], sems[2:4], sems[4:6], sems[6], sems[7]
        self.at = place()
        self.core = self.at['core']
        self.other = moved(self.at, 'core', 1)
        self.around = [moved(self.at, d, s) for d in 'xyz' for s in (LEFT, RIGHT)]
        greet([self.other] + self.around)
        self.rings = {}
        for t in (Q, D):
            for k, (first, rows) in enumerate(COLOURS):
                dims = ORDERS[t][k]
                base = self.core * HALF + first
                for p in (OUTER, MIDDLE, INNER):
                    n = rows * RING_SIZE[p]
                    index = (t * len(COLOURS) + k) * len(RING_SIZE) + p
                    self.rings[t, k, p] = Ring(self.at, dims[p], acc.at[t], base, n, bufs[p], 3 * first // SIDE ** (p + 1), self.ring_sems, index)
                    base = base + self.at[dims[p]] * n

    def met(self):
        pl.semaphore_wait(pltpu.get_barrier_semaphore(), len(self.around) + 1)

    def level(self, t, p):
        return [self.rings[t, k, p] for k in range(len(COLOURS))]

    def pair_copy(self, t, rel, k):
        first, ring = COLOURS[k][0], self.rings[t, k, OUTER]
        spot = ring.spot[rel] + (1 - self.core * 2) * HALF
        dst = self.pair.at[PAIR_SLOT[rel], pl.ds(first // SIDE, ring.n)]
        return remote(self.acc.at[t, pl.ds(spot, ring.n)], dst, self.pair_sems, t * 12 + rel * 3 + k, self.other)

    def pairs(self, t, rel, fresh=False):
        if not fresh:
            pl.semaphore_wait(self.credit.at[PAIR_SLOT[rel]], 1)
        for k in range(len(COLOURS)):
            self.pair_copy(t, rel, k).start()

    def settle(self, t, rel, last=False):
        for k, ring in enumerate(self.level(t, OUTER)):
            self.pair_copy(t, rel, k).wait_recv()
            add_into(ring.x, ring.spot[rel], [(self.pair.at[PAIR_SLOT[rel]], COLOURS[k][0] // SIDE)], ring.n)
        if not last:
            pl.semaphore_signal(self.credit.at[PAIR_SLOT[rel]], inc=1, device_id=device(self.other), device_id_type=MESH)

    def start(self, t, p, which):
        for ring in self.level(t, p):
            ring.start(which)

    def rs_pass(self, t, p):
        for ring in self.level(t, p):
            ring.rs_pass()

    def rs_end(self, t, p):
        for ring in self.level(t, p):
            ring.rs_end()
        for k, ring in enumerate(self.level(t, p)):
            ring.sent(FAR + NEAR + ON)
            for rel in range(SIDE) if p == OUTER else ():
                self.pair_copy(t, rel, k).wait_send()
        for peer in self.around:
            pl.semaphore_signal(self.ready.at[t * 3 + p], inc=1, device_id=device(peer), device_id_type=MESH)
        if p == OUTER:
            pl.semaphore_signal(self.ready.at[6 + t], inc=1, device_id=device(self.other), device_id_type=MESH)

    def opened(self, t, p):
        pl.semaphore_wait(self.ready.at[t * 3 + p], len(self.around))

    def hand(self, t, k, p, rel, second):
        ring = self.rings[t, k, p]
        shift, size = (0, ring.n) if rel != ACROSS else (ring.half, ring.rest) if second else (0, ring.half)
        here = self.acc.at[t, pl.ds(ring.spot[rel] + shift, size)]
        kind = HANDS.index((rel, second))
        return remote(here, here, self.hand_sems, ((t * 3 + k) * 3 + p) * len(HANDS) + kind, self.other)

    def ag_start(self, t, p, which=FIRST + SECOND):
        self.start(t, p, which)
        if p == INNER:
            pl.semaphore_wait(self.ready.at[6 + t], 1)
            for k in range(len(COLOURS)):
                self.hand(t, k, p, OWN, False).start()

    def ag_pass(self, t, p):
        for ring in self.level(t, p):
            ring.ag_pass()
        for k, ring in enumerate(self.level(t, p)):
            for m, rel in zip(SECOND, (LEFT, RIGHT)):
                ring.take((m,))
                self.hand(t, k, p, rel, False).start()

    def ag_end(self, t, p):
        for k, ring in enumerate(self.level(t, p)):
            for m, second in zip(ONWARD, (False, True)):
                ring.take((m,))
                self.hand(t, k, p, ACROSS, second).start()

    def finish(self):
        hands = [(t, k, p, *h) for t, k, p in self.rings for h in HANDS if h[0] != OWN or p == INNER]
        for h in hands:
            self.hand(*h).wait_recv()
        for ring in self.rings.values():
            ring.sent(GATHER)
        for h in hands:
            self.hand(*h).wait_send()


def train_kernel(q_hbm, d_hbm, ups_hbm, q_w1, q_w2, q_proj, d_w1, d_w2, d_proj, acc, w_one, w_two, w_proj, pre_s, act_s, pair, q_in, d_in, ups, in_sems, *rest):
    q_up, d_up = up_rows(ups)
    bufs, w_sems, sems = rest[:3], rest[3], rest[4:]
    loads = arrivals(((q_hbm, q_in), (d_hbm, d_in), (ups_hbm, ups)), in_sems)
    ex = Exchange(acc, pair, bufs, sems)

    held = (w_one, w_two, w_proj)
    q_loads, d_loads = weight_loads((q_w1, q_w2, q_proj), held, w_sems), weight_loads((d_w1, d_w2, d_proj), held, w_sems)
    for c in q_loads:
        c.start()

    def at_hooks(sub, table):
        def hook(i):
            for when, work in table:
                if when[1] == i:
                    if isinstance(sub, int):
                        work() if sub == when[0] else None
                    else:
                        pl.when(sub == when[0])(work)

        return hook

    def swap_early():
        d_loads[0].start()

    def swap_late():
        for c in d_loads[2:]:
            c.start()

    def q_body(sub, carry):
        hook = at_hooks(sub, (((3, 1), swap_early), ((3, 2), swap_late)))
        tower_backward(sub, 16, q_in, q_up, *held, acc.at[Q], pre_s, act_s, hook)
        return carry

    for c in loads:
        c.wait()
    tower_backward(0, 16, q_in, q_up, *held, acc.at[Q], pre_s, act_s, lambda i: None, lambda step: q_loads[step].wait())
    lax.fori_loop(1, SUB_COUNT, q_body, 0)
    d_loads[1].start()
    ex.met()
    ex.pairs(Q, ACROSS, fresh=True)
    ex.pairs(Q, RIGHT, fresh=True)
    def across():
        ex.settle(Q, ACROSS)
        ex.start(Q, OUTER, FAR)

    def right():
        ex.pairs(Q, LEFT)
        ex.settle(Q, RIGHT)

    def left():
        ex.settle(Q, LEFT)
        ex.start(Q, OUTER, NEAR)

    def own():
        ex.settle(Q, OWN)
        ex.rs_pass(Q, OUTER)

    steps = (
        ((0, 2), across), ((0, 3), right),
        ((1, 1), functools.partial(ex.pairs, Q, OWN)), ((1, 2), left), ((1, 3), own),
    )

    def d_body(sub, carry):
        tower_backward(sub, 32, d_in, d_up, *held, acc.at[D], pre_s, act_s, at_hooks(sub, steps))
        return carry

    tower_backward(0, 32, d_in, d_up, *held, acc.at[D], pre_s, act_s, at_hooks(0, steps), lambda step: d_loads[step].wait())
    lax.fori_loop(1, SUB_COUNT, d_body, 0)
    ex.pairs(D, ACROSS)
    ex.pairs(D, RIGHT)
    ex.rs_end(Q, OUTER)
    ex.start(Q, MIDDLE, FAR + NEAR)
    ex.settle(D, ACROSS)
    ex.pairs(D, LEFT)
    ex.rs_pass(Q, MIDDLE)
    ex.opened(Q, OUTER)
    ex.start(D, OUTER, FAR)
    ex.settle(D, RIGHT)
    ex.pairs(D, OWN)
    ex.rs_end(Q, MIDDLE)
    ex.start(Q, INNER, FAR + NEAR)
    ex.settle(D, LEFT, last=True)
    ex.start(D, OUTER, NEAR)
    ex.settle(D, OWN, last=True)
    ex.rs_pass(Q, INNER)
    ex.rs_pass(D, OUTER)
    ex.rs_end(Q, INNER)
    ex.opened(Q, INNER)
    ex.ag_start(Q, INNER)
    ex.rs_end(D, OUTER)
    ex.opened(Q, MIDDLE)
    ex.start(D, MIDDLE, FAR + NEAR)
    ex.ag_pass(Q, INNER)
    ex.ag_end(Q, INNER)
    ex.ag_start(Q, MIDDLE)
    ex.rs_pass(D, MIDDLE)
    ex.ag_pass(Q, MIDDLE)
    ex.rs_end(D, MIDDLE)
    ex.start(D, INNER, FAR + NEAR)
    ex.ag_end(Q, MIDDLE)
    ex.ag_start(Q, OUTER, FIRST)
    ex.rs_pass(D, INNER)
    ex.rs_end(D, INNER)
    ex.opened(D, INNER)
    ex.ag_start(D, INNER)
    ex.ag_start(Q, OUTER, SECOND)
    ex.ag_pass(D, INNER)
    ex.ag_pass(Q, OUTER)
    ex.ag_end(D, INNER)
    ex.opened(D, MIDDLE)
    ex.ag_start(D, MIDDLE)
    ex.ag_pass(D, MIDDLE)
    ex.ag_end(Q, OUTER)
    ex.ag_end(D, MIDDLE)
    ex.opened(D, OUTER)
    ex.ag_start(D, OUTER)
    ex.ag_pass(D, OUTER)
    ex.ag_end(D, OUTER)
    ex.finish()


def train(q_rows, d_rows, ups, weights):
    vmem, whole = pl.BlockSpec(memory_space=pltpu.VMEM), pl.BlockSpec(memory_space=pl.ANY)
    bufs = [pltpu.VMEM((3 * HALF // SIDE ** p // SIDE, 8, COLS), F32) for p in (OUTER, MIDDLE, INNER)]
    dma = pltpu.SemaphoreType.DMA
    return pl.pallas_call(
        train_kernel,
        out_shape=pltpu.VMEM((2, UNITS, 8, COLS), F32),
        in_specs=[whole] * 9,
        out_specs=vmem,
        scratch_shapes=[
            *[pltpu.VMEM(shape, BF16) for shape in WEIGHT_SHAPES],
            pltpu.VMEM((2, 32, FFN), F32),
            pltpu.VMEM((2, 32, FFN), BF16),
            pltpu.VMEM((2, 272, 8, COLS), F32),
            pltpu.VMEM(q_rows.shape, BF16),
            pltpu.VMEM(d_rows.shape, BF16),
            pltpu.VMEM(ups.shape, BF16),
            pltpu.SemaphoreType.DMA((3,)),
            *bufs,
            dma((5,)), *[dma((n,)) for n in (24, 24, 216, 216, 90, 90)],
            pltpu.SemaphoreType.REGULAR((2,)), pltpu.SemaphoreType.REGULAR((8,)),
        ],
        compiler_params=pltpu.CompilerParams(collective_id=1, has_side_effects=True, vmem_limit_bytes=TRAIN_VMEM),
        name='towers_backward_all_reduce',
    )(q_rows, d_rows, ups, *weights)


def unpack_kernel(acc, *rest):
    outs, sem = rest[:6], rest[6]
    copies = []
    for t in range(2):
        one, two, proj = outs[t * 3:t * 3 + 3]
        for k in range(2):
            for c in range(8):
                copies.append((acc.at[t, pl.ds(k * DIM + c * 64, 64)], one.at[k, :, :, pl.ds(c * COLS, COLS)]))
            for c in range(2):
                copies.append((acc.at[t, pl.ds(1024 + k * DIM + c * COLS, COLS)], two.at[k, :, :, pl.ds(c * COLS, COLS)]))
        for c in range(2):
            copies.append((acc.at[t, pl.ds(FFN + c * 64, 64)], proj.at[:, :, pl.ds(c * COLS, COLS)]))
    copies = [pltpu.make_async_copy(src, dst, sem.at[i]) for i, (src, dst) in enumerate(copies)]
    for c in copies:
        c.start()
    for c in copies:
        c.wait()


def unpack(acc):
    shapes = ((2, 64, 8, FFN), (2, COLS, 8, DIM), (64, 8, DIM)) * 2
    outs = pl.pallas_call(
        unpack_kernel,
        out_shape=tuple(jax.ShapeDtypeStruct(s, F32) for s in shapes),
        in_specs=[pl.BlockSpec(memory_space=pltpu.VMEM)],
        out_specs=(pl.BlockSpec(memory_space=pl.ANY),) * 6,
        scratch_shapes=[pltpu.SemaphoreType.DMA((44,))],
        compiler_params=pltpu.CompilerParams(vmem_limit_bytes=1 << 20),
        name='unpack',
    )(acc)
    return tuple(o.reshape(s) for o, s in zip(outs, WEIGHT_SHAPES * 2))


def local_step(q_loc, d_loc, temperature, *weights):
    d_rows = d_loc.reshape(-1, d_loc.shape[-1])
    ups, loss = scores(temperature.reshape(1), q_loc, d_rows, weights)
    return (loss.reshape(()), *unpack(train(q_loc, d_rows, ups, weights)))


def solution(mesh):
    specs_in = (P('data', None), P(None, 'data', None), P(), P(), P(), P(), P(), P(), P())
    specs_out = (P(), P(), P(), P(), P(), P(), P())
    return jax.shard_map(local_step, mesh=mesh, in_specs=specs_in, out_specs=specs_out, check_vma=False)
```

```python
import functools

import jax
import jax.numpy as jnp
from jax import lax
from jax.experimental import pallas as pl
from jax.experimental.pallas import tpu as pltpu
from jax.sharding import PartitionSpec as P

F32 = jnp.float32
BF16 = jnp.bfloat16
MESH = pl.DeviceIdType.MESH
SUB_COUNT = 4
SIDE = 4
ROWS_CONTRACT = (((0,), (0,)), ((), ()))
LAST_CONTRACT = (((1,), (1,)), ((), ()))
SCORE_VMEM = 67043328

UNITS = 2176
HALF = 1088
TRAIN_VMEM = 27500000
PAIR_SLOT = (1, 1, 0, 0)
RING_SIZE = (16, 4, 1)
Q, D = range(2)
OUTER, MIDDLE, INNER = range(3)
OWN, RIGHT, ACROSS, LEFT = range(4)
MESSAGES = (
    (ACROSS, False, 0, 0), (ACROSS, True, 1, 0), (RIGHT, True, 0, 1), (LEFT, False, 1, 2), (RIGHT, False, 0, 1), (LEFT, True, 1, 2),
    (OWN, False, 0, None), (OWN, True, 1, None), (OWN, True, 0, None), (OWN, False, 1, None), (LEFT, False, 0, None), (RIGHT, True, 1, None),
)
ALL = tuple(range(len(MESSAGES)))
FAR, NEAR, ON, GATHER = ALL[:2], ALL[2:4], ALL[4:6], ALL[6:]
FIRST, SECOND, ONWARD = GATHER[:2], GATHER[2:4], GATHER[4:]
DIM, FFN, COLS = 512, 2048, 256
WEIGHT_SHAPES = ((2, DIM, FFN), (2, FFN, DIM), (DIM, DIM))
COLOURS = ((0, 6), (384, 6), (768, 5))
ORDERS = (('xyz', 'yzx', 'zxy'), ('zxy', 'xyz', 'yzx'))
HANDS = ((LEFT, False), (RIGHT, False), (ACROSS, False), (ACROSS, True), (OWN, False))


def place():
    me = lax.axis_index('data')
    core = lax.rem(me, 2)
    x = lax.rem(me // 2, SIDE)
    y = lax.rem(me // 8, SIDE)
    z = me // 32
    return dict(z=z, y=y, x=x, core=core)


def device(at):
    return (((at['z'] * SIDE + at['y']) * SIDE + at['x']) * 2 + at['core'],)


def moved(at, dim, step):
    size = 2 if dim == 'core' else SIDE
    return {**at, dim: lax.rem(at[dim] + step, size)}


def remote(src, dst, sems, index, peer):
    return pltpu.make_async_remote_copy(
        src_ref=src, dst_ref=dst, send_sem=sems[0].at[index], recv_sem=sems[1].at[index], device_id=device(peer), device_id_type=MESH
    )


def greet(peers):
    for peer in peers:
        pl.semaphore_signal(pltpu.get_barrier_semaphore(), inc=1, device_id=device(peer), device_id_type=MESH)


def dot(lhs, rhs, dims=None):
    if dims is None:
        return jnp.dot(lhs, rhs, preferred_element_type=F32)
    return lax.dot_general(lhs, rhs, dims, preferred_element_type=F32)


def add_into(dst, dst_at, pieces, size):
    step = next(s for s in (16, 12, 10, 8, 6, 5, 4, 3, 2, 1) if size % s == 0)

    def body(i, carry):
        here = pl.ds(dst_at + i * step, step)
        total = dst[here]
        for ref, ref_at in pieces:
            total = total + ref[pl.ds(ref_at + i * step, step)]
        dst[here] = total
        return carry

    lax.fori_loop(0, size // step, body, 0)


class Ring:
    def __init__(self, at, dim, x, base, n, buf, buf_at, sems, sem_at):
        self.x, self.n, self.buf, self.buf_at = x, n, buf, buf_at
        self.half = (n + 1) // 2
        self.rest = n - self.half
        self.spot = [base + lax.rem(at[dim] + rel, SIDE) * n for rel in range(SIDE)]
        self.peers = moved(at, dim, RIGHT), moved(at, dim, LEFT)
        self.sems, self.sem_at = sems, sem_at * len(MESSAGES)

    def copy(self, m):
        rel, second, way, slot = MESSAGES[m]
        shift, size = (self.half, self.rest) if second else (0, self.half)
        src = self.x.at[pl.ds(self.spot[rel] + shift, size)]
        dst = src if slot is None else self.buf.at[pl.ds(self.buf_at + slot * self.n + shift, size)]
        return remote(src, dst, self.sems, self.sem_at + m, self.peers[way])

    def start(self, which):
        for m in which:
            self.copy(m).start()

    def take(self, which):
        for m in which:
            self.copy(m).wait_recv()

    def sent(self, which):
        for m in which:
            self.copy(m).wait_send()

    def rs_pass(self):
        self.take(FAR[:1])
        add_into(self.x, self.spot[RIGHT], [(self.buf, self.buf_at)], self.half)
        self.start(ON[:1])
        self.take(FAR[1:])
        add_into(self.x, self.spot[LEFT] + self.half, [(self.buf, self.buf_at + self.half)], self.rest)
        self.start(ON[1:])

    def rs_end(self):
        self.take(NEAR + ON)
        got = [(self.buf, self.buf_at + slot * self.n) for slot in (1, 2)]
        add_into(self.x, self.spot[OWN], got, self.n)

    def ag_pass(self):
        for first, then in zip(GATHER[:2], GATHER[4:]):
            self.copy(first).wait_recv()
            self.copy(then).start()


def tower_forward(rows, w_one, w_two, w_proj, ready):
    hidden = rows
    for layer in range(2):
        ready(2 * layer)
        act = jax.nn.gelu(dot(hidden, w_one[layer])).astype(BF16)
        ready(2 * layer + 1)
        hidden = (hidden.astype(F32) + dot(act, w_two[layer])).astype(BF16)
    ready(4)
    return dot(hidden, w_proj[...]).astype(BF16)


def up_rows(ups):
    return ups.at[pl.ds(0, 64)], ups.at[pl.ds(64, 128)]


def arrivals(pairs, sems):
    copies = [pltpu.make_async_copy(src, dst, sems.at[i]) for i, (src, dst) in enumerate(pairs)]
    for c in copies:
        c.start()
    return copies


def weight_loads(src, dst, sems, at=0):
    pairs = [(one.at[layer], two.at[layer]) for layer in range(2) for one, two in zip(src[:2], dst[:2])]
    return [pltpu.make_async_copy(one, two, sems.at[at + i]) for i, (one, two) in enumerate(pairs + [(src[2], dst[2])])]


def score_kernel(
    tau_ref, q_ref, d_ref, q_w1, q_w2, q_proj, d_w1, d_w2, d_proj, ups, loss_ref,
    q_all, d_all, st, stats, q_part, d_part, q_buf, d_buf, pair, loss_all, loss_row, q_one, q_two, q_last, d_one, d_two, d_last, w_sems, *sems
):
    q_weights, d_weights = (q_one, q_two, q_last), (d_one, d_two, d_last)
    q_loads = weight_loads((q_w1, q_w2, q_proj), q_weights, w_sems)
    d_loads = weight_loads((d_w1, d_w2, d_proj), d_weights, w_sems, len(q_loads))
    for c in q_loads + d_loads:
        c.start()
    q_up, d_up = up_rows(ups)
    at = place()
    core, z = at['core'], at['z']
    other = moved(at, 'core', 1)
    q_peers = [moved(moved(at, 'x', s % SIDE), 'y', s // SIDE) for s in range(1, 16)]
    d_peers = [moved(moved(at, 'core', s % 2), 'z', s // 2) for s in range(1, 8)]
    q_slot, d_slot = at['y'] * SIDE + at['x'], core * SIDE + z
    greet(q_peers + d_peers)

    outer, inner = ('y', 'x'), ('x', 'y')
    own = [at[outer[h]] * 8 + at[inner[h]] * 2 for h in range(2)]

    def q_rings(x, h):
        wide = Ring(at, outer[h], x.at[h], 0, 8, q_buf.at[h], 0, sems, h)
        return wide, Ring(at, inner[h], x.at[h], at[outer[h]] * 8, 2, q_buf.at[h], 24, sems, 2 + h)

    q_wide, q_thin = zip(*[q_rings(q_all, h) for h in range(2)])
    docs_ring = Ring(at, 'z', d_all.at[core], 0, 8, d_buf, 0, sems, 4)
    hands_at = 5 * len(MESSAGES)
    def hand(rel):
        here = d_all.at[core, pl.ds(docs_ring.spot[rel], 8)]
        return remote(here, here, sems, hands_at + rel, other)

    used = [hands_at + SIDE + 1]

    def broadcast(src, peers):
        copies = [remote(src, src, sems, used[0] + i, p) for i, p in enumerate(peers)]
        used[0] += len(peers)
        for c in copies:
            c.start()
        return copies

    for h in range(2):
        def q_body(i, carry):
            def ready(step):
                if h == 0:
                    pl.when(i == 0)(q_loads[step].wait)

            rows = pl.ds(pl.multiple_of((h * 2 + i) * 16, 16), 16)
            q_all[h, own[h] + i] = tower_forward(q_ref[rows, :], *q_weights, ready)
            return carry

        lax.fori_loop(0, 2, q_body, 0)
        if h == 0:
            pl.semaphore_wait(pltpu.get_barrier_semaphore(), len(q_peers) + len(d_peers))
        q_thin[h].start(FIRST + SECOND)
    for c in d_loads:
        c.wait()

    def d_body(i, carry):
        rows = pl.ds(pl.multiple_of(i * 32, 32), 32)
        d_all[core, pl.ds(z * 8 + i * 2, 2)] = tower_forward(d_ref[rows, :], *d_weights, lambda step: None).reshape(2, 16, DIM)

        @pl.when(i == 1)
        def _():
            docs_ring.start(FIRST[:1] + SECOND[1:])
            for ring in q_thin:
                ring.ag_pass()

        @pl.when(i == 2)
        def _():
            for thin, wide in zip(q_thin, q_wide):
                thin.take(SECOND + ONWARD)
                wide.start(FIRST + SECOND)

        return carry

    lax.fori_loop(0, SUB_COUNT, d_body, 0)
    docs_ring.start(FIRST[1:] + SECOND[:1])
    hand(OWN).start()
    docs_ring.take(FIRST[:1])
    docs_ring.start(ONWARD[:1])
    for ring in q_wide:
        ring.ag_pass()
    docs_ring.take(FIRST[1:])
    docs_ring.start(ONWARD[1:])
    docs_ring.take(SECOND)
    hand(LEFT).start()
    hand(RIGHT).start()
    docs_ring.take(ONWARD)
    hand(ACROSS).start()
    for ring in q_wide:
        ring.take(SECOND + ONWARD)
    for rel in range(SIDE):
        hand(rel).wait_recv()

    tau = tau_ref[0]
    queries = q_all[...].reshape(1024, DIM)
    docs = d_all[...].reshape(1024, DIM)
    highs = []
    for b in range(2):
        rows = slice(b * DIM, (b + 1) * DIM)
        tile = dot(docs[rows], queries, LAST_CONTRACT) / tau
        st[rows] = tile
        highs.append(jnp.max(tile, axis=0, keepdims=True))
    high = functools.reduce(jnp.maximum, highs)
    blocks = [slice(b * 128, (b + 1) * 128) for b in range(8)]
    total = sum(jnp.sum(jnp.exp(st[rows] - high), axis=0, keepdims=True) for rows in blocks)
    stats[q_slot] = high + jnp.log(total)
    shares = broadcast(stats.at[q_slot], q_peers)
    for c in shares:
        c.wait_recv()
    all_stats = [stats[j] for j in range(16)]
    top = functools.reduce(jnp.maximum, all_stats)
    log_norm = top + jnp.log(sum(jnp.exp(part - top) for part in all_stats))

    def matches(rows):
        row = lax.broadcasted_iota(jnp.int32, (rows, 1024), 0)
        column = lax.broadcasted_iota(jnp.int32, (rows, 1024), 1)
        return (row < 64) & (column == jnp.where(row < 32, own[0] * 16 + row, 480 + own[1] * 16 + row))

    def spread(values):
        return jnp.broadcast_to(jnp.sum(values, keepdims=True), (1, 128))

    positive = st[pl.ds(pl.multiple_of(d_slot * 128, 128), 64), :]
    loss_all[d_slot] = spread(jnp.where(matches(64), log_norm - positive, 0.0))
    losses = broadcast(loss_all.at[d_slot], d_peers)

    scale = 8192.0 * tau
    hit = matches(128)
    grads = []
    for b, rows in enumerate(blocks):
        soft = jnp.exp(st[rows] - log_norm) - jnp.where(hit & (d_slot == b), 1.0, 0.0)
        grads.append((soft / scale).astype(BF16))
    grad = jnp.concatenate(grads, axis=0)
    q_wide, q_thin = zip(*[q_rings(q_part, h) for h in range(2)])
    for h in range(2):
        q_part[h] = dot(grad[:, h * DIM:(h + 1) * DIM], docs, ROWS_CONTRACT).reshape(32, 16, DIM)
        q_wide[h].start(FAR + NEAR)
    for c in range(2):
        d_part[c] = dot(grad[c * DIM:(c + 1) * DIM], queries).reshape(32, 16, DIM)
    swap = remote(d_part.at[other['core']], pair, sems, hands_at + SIDE, other)
    swap.start()
    docs_sum = Ring(at, 'z', d_part.at[core], 0, 8, d_buf, 0, sems, 4)
    q_wide[0].rs_pass()
    swap.wait_recv()
    add_into(d_part.at[core], 0, [(pair, 0)], 32)
    docs_sum.start(FAR + NEAR)
    q_wide[1].rs_pass()
    for wide, thin in zip(q_wide, q_thin):
        wide.rs_end()
        thin.start(FAR + NEAR)
    docs_sum.rs_pass()
    for c in losses:
        c.wait_recv()
    loss_row[q_slot] = sum(loss_all[j] for j in range(8))
    row_losses = broadcast(loss_row.at[q_slot], q_peers)
    for ring in q_thin:
        ring.rs_pass()
    for h, ring in enumerate(q_thin):
        ring.rs_end()
        q_up[h * 32:(h + 1) * 32, :] = q_part[h, pl.ds(own[h], 2)].reshape(32, DIM).astype(BF16)
    docs_sum.rs_end()
    for c in row_losses:
        c.wait_recv()
    loss_ref[...] = sum(loss_row[j, :, 0:1] for j in range(16)) / 8192.0
    d_up[...] = d_part[core, pl.ds(z * 8, 8)].reshape(128, DIM).astype(BF16)
    for c in shares + losses + row_losses + [swap] + list(map(hand, range(SIDE))):
        c.wait_send()
    for ring in (*q_wide, *q_thin, docs_sum):
        ring.sent(FAR + NEAR + ON)
    for h in range(2):
        for ring in q_rings(q_all, h):
            ring.sent(GATHER)
    docs_ring.sent(GATHER)


def scores(tau, q_rows, d_rows, weights):
    vmem, whole = pl.BlockSpec(memory_space=pltpu.VMEM), pl.BlockSpec(memory_space=pl.ANY)
    copies = 5 * len(MESSAGES) + 42
    return pl.pallas_call(
        score_kernel,
        out_shape=(jax.ShapeDtypeStruct((192, DIM), BF16), jax.ShapeDtypeStruct((1, 1), F32)),
        in_specs=[pl.BlockSpec(memory_space=pltpu.SMEM), vmem, vmem] + [whole] * 6,
        out_specs=(vmem,) * 2,
        scratch_shapes=[
            pltpu.VMEM((2, 32, 16, DIM), BF16),
            pltpu.VMEM((2, 32, 16, DIM), BF16),
            pltpu.VMEM((1024, 1024), F32),
            pltpu.VMEM((16, 1, 1024), F32),
            pltpu.VMEM((2, 32, 16, DIM), F32),
            pltpu.VMEM((2, 32, 16, DIM), F32),
            pltpu.VMEM((2, 30, 16, DIM), F32),
            pltpu.VMEM((24, 16, DIM), F32),
            pltpu.VMEM((32, 16, DIM), F32),
            pltpu.VMEM((8, 1, 128), F32),
            pltpu.VMEM((16, 1, 128), F32),
            *[pltpu.VMEM(shape, BF16) for shape in WEIGHT_SHAPES * 2],
            pltpu.SemaphoreType.DMA((10,)),
            pltpu.SemaphoreType.DMA((copies,)),
            pltpu.SemaphoreType.DMA((copies,)),
        ],
        compiler_params=pltpu.CompilerParams(collective_id=0, has_side_effects=True, vmem_limit_bytes=SCORE_VMEM),
        name='towers_forward_scores',
    )(tau, q_rows, d_rows, *weights)


def gelu_back(pre, act_grad):
    return jax.vjp(jax.nn.gelu, pre)[1](act_grad)[0]


def tower_backward(sub, rows_per, x_ref, up_ref, w_one, w_two, w_proj, acc, pre_s, act_s, hook, ready=None):
    first = ready is not None
    rows = pl.ds(0 if first else pl.multiple_of(sub * rows_per, rows_per), rows_per)
    ready = ready or (lambda step: None)
    hidden = [x_ref[rows, :]]
    for layer in range(2):
        ready(2 * layer)
        pre = dot(hidden[layer], w_one[layer])
        pre_s[layer, 0:rows_per] = pre
        act = jax.nn.gelu(pre).astype(BF16)
        act_s[layer, 0:rows_per] = act
        ready(2 * layer + 1)
        hidden.append((hidden[layer].astype(F32) + dot(act, w_two[layer])).astype(BF16))
    ready(4)
    hook(1)
    up = up_ref[rows, :]

    def add(base, stride, lhs, rhs):
        for i in range(lhs.shape[1] // COLS):
            part = dot(lhs[:, i * COLS:(i + 1) * COLS], rhs, ROWS_CONTRACT)
            for j in range(2):
                spot = base + j * stride + i * 32
                tile = part[:, j * COLS:(j + 1) * COLS].reshape(32, 8, COLS)
                acc[spot:spot + 32] = tile if first else acc[spot:spot + 32] + tile

    add(FFN, 64, hidden[2], up)
    resid = dot(up, w_proj[...], LAST_CONTRACT)
    for layer in (1, 0):
        resid_bf = resid.astype(BF16)
        add(1024 + layer * DIM, COLS, act_s[layer, 0:rows_per], resid_bf)
        act_grad = dot(resid_bf, w_two[layer], LAST_CONTRACT)
        pre_grad = gelu_back(pre_s[layer, 0:rows_per], act_grad).astype(BF16)
        for c in range(4):
            add(layer * DIM + c * 128, 64, hidden[layer], pre_grad[:, c * DIM:(c + 1) * DIM])
        if layer == 1:
            resid = resid + dot(pre_grad, w_one[layer], LAST_CONTRACT)
            hook(2)
    hook(3)


class Exchange:
    def __init__(self, acc, pair, bufs, sems):
        self.acc, self.pair = acc, pair
        self.pair_sems, self.ring_sems, self.hand_sems, self.credit, self.ready = sems[:2], sems[2:4], sems[4:6], sems[6], sems[7]
        self.at = place()
        self.core = self.at['core']
        self.other = moved(self.at, 'core', 1)
        self.around = [moved(self.at, d, s) for d in 'xyz' for s in (LEFT, RIGHT)]
        greet([self.other] + self.around)
        self.rings = {}
        for t in (Q, D):
            for k, (first, rows) in enumerate(COLOURS):
                dims = ORDERS[t][k]
                base = self.core * HALF + first
                for p in (OUTER, MIDDLE, INNER):
                    n = rows * RING_SIZE[p]
                    index = (t * len(COLOURS) + k) * len(RING_SIZE) + p
                    self.rings[t, k, p] = Ring(self.at, dims[p], acc.at[t], base, n, bufs[p], 3 * first // SIDE ** (p + 1), self.ring_sems, index)
                    base = base + self.at[dims[p]] * n

    def met(self):
        pl.semaphore_wait(pltpu.get_barrier_semaphore(), len(self.around) + 1)

    def level(self, t, p):
        return [self.rings[t, k, p] for k in range(len(COLOURS))]

    def pair_copy(self, t, rel, k):
        first, ring = COLOURS[k][0], self.rings[t, k, OUTER]
        spot = ring.spot[rel] + (1 - self.core * 2) * HALF
        dst = self.pair.at[PAIR_SLOT[rel], pl.ds(first // SIDE, ring.n)]
        return remote(self.acc.at[t, pl.ds(spot, ring.n)], dst, self.pair_sems, t * 12 + rel * 3 + k, self.other)

    def pairs(self, t, rel, fresh=False):
        if not fresh:
            pl.semaphore_wait(self.credit.at[PAIR_SLOT[rel]], 1)
        for k in range(len(COLOURS)):
            self.pair_copy(t, rel, k).start()

    def settle(self, t, rel, last=False):
        for k, ring in enumerate(self.level(t, OUTER)):
            self.pair_copy(t, rel, k).wait_recv()
            add_into(ring.x, ring.spot[rel], [(self.pair.at[PAIR_SLOT[rel]], COLOURS[k][0] // SIDE)], ring.n)
        if not last:
            pl.semaphore_signal(self.credit.at[PAIR_SLOT[rel]], inc=1, device_id=device(self.other), device_id_type=MESH)

    def start(self, t, p, which):
        for ring in self.level(t, p):
            ring.start(which)

    def rs_pass(self, t, p):
        for ring in self.level(t, p):
            ring.rs_pass()

    def rs_end(self, t, p):
        for ring in self.level(t, p):
            ring.rs_end()
        for k, ring in enumerate(self.level(t, p)):
            ring.sent(FAR + NEAR + ON)
            for rel in range(SIDE) if p == OUTER else ():
                self.pair_copy(t, rel, k).wait_send()
        for peer in self.around:
            pl.semaphore_signal(self.ready.at[t * 3 + p], inc=1, device_id=device(peer), device_id_type=MESH)
        if p == OUTER:
            pl.semaphore_signal(self.ready.at[6 + t], inc=1, device_id=device(self.other), device_id_type=MESH)

    def opened(self, t, p):
        pl.semaphore_wait(self.ready.at[t * 3 + p], len(self.around))

    def hand(self, t, k, p, rel, second):
        ring = self.rings[t, k, p]
        shift, size = (0, ring.n) if rel != ACROSS else (ring.half, ring.rest) if second else (0, ring.half)
        here = self.acc.at[t, pl.ds(ring.spot[rel] + shift, size)]
        kind = HANDS.index((rel, second))
        return remote(here, here, self.hand_sems, ((t * 3 + k) * 3 + p) * len(HANDS) + kind, self.other)

    def ag_start(self, t, p, which=FIRST + SECOND):
        self.start(t, p, which)
        if p == INNER:
            pl.semaphore_wait(self.ready.at[6 + t], 1)
            for k in range(len(COLOURS)):
                self.hand(t, k, p, OWN, False).start()

    def ag_pass(self, t, p):
        for ring in self.level(t, p):
            ring.ag_pass()
        for k, ring in enumerate(self.level(t, p)):
            for m, rel in zip(SECOND, (LEFT, RIGHT)):
                ring.take((m,))
                self.hand(t, k, p, rel, False).start()

    def ag_end(self, t, p):
        for k, ring in enumerate(self.level(t, p)):
            for m, second in zip(ONWARD, (False, True)):
                ring.take((m,))
                self.hand(t, k, p, ACROSS, second).start()

    def finish(self):
        hands = [(t, k, p, *h) for t, k, p in self.rings for h in HANDS if h[0] != OWN or p == INNER]
        for h in hands:
            self.hand(*h).wait_recv()
        for ring in self.rings.values():
            ring.sent(GATHER)
        for h in hands:
            self.hand(*h).wait_send()


def train_kernel(q_hbm, d_hbm, ups_hbm, q_w1, q_w2, q_proj, d_w1, d_w2, d_proj, acc, w_one, w_two, w_proj, pre_s, act_s, pair, q_in, d_in, ups, in_sems, *rest):
    q_up, d_up = up_rows(ups)
    bufs, w_sems, sems = rest[:3], rest[3], rest[4:]
    loads = arrivals(((q_hbm, q_in), (d_hbm, d_in), (ups_hbm, ups)), in_sems)
    ex = Exchange(acc, pair, bufs, sems)

    held = (w_one, w_two, w_proj)
    q_loads, d_loads = weight_loads((q_w1, q_w2, q_proj), held, w_sems), weight_loads((d_w1, d_w2, d_proj), held, w_sems)
    for c in q_loads:
        c.start()

    def at_hooks(sub, table):
        def hook(i):
            for when, work in table:
                if when[1] == i:
                    if isinstance(sub, int):
                        work() if sub == when[0] else None
                    else:
                        pl.when(sub == when[0])(work)

        return hook

    def swap_early():
        d_loads[0].start()

    def swap_late():
        for c in d_loads[2:]:
            c.start()

    def q_body(sub, carry):
        hook = at_hooks(sub, (((3, 1), swap_early), ((3, 2), swap_late)))
        tower_backward(sub, 16, q_in, q_up, *held, acc.at[Q], pre_s, act_s, hook)
        return carry

    for c in loads:
        c.wait()
    tower_backward(0, 16, q_in, q_up, *held, acc.at[Q], pre_s, act_s, lambda i: None, lambda step: q_loads[step].wait())
    lax.fori_loop(1, SUB_COUNT, q_body, 0)
    d_loads[1].start()
    ex.met()
    ex.pairs(Q, ACROSS, fresh=True)
    ex.pairs(Q, RIGHT, fresh=True)
    def across():
        ex.settle(Q, ACROSS)
        ex.start(Q, OUTER, FAR)

    def right():
        ex.pairs(Q, LEFT)
        ex.settle(Q, RIGHT)

    def left():
        ex.settle(Q, LEFT)
        ex.start(Q, OUTER, NEAR)

    def own():
        ex.settle(Q, OWN)
        ex.rs_pass(Q, OUTER)

    steps = (
        ((0, 2), across), ((0, 3), right),
        ((1, 1), functools.partial(ex.pairs, Q, OWN)), ((1, 2), left), ((1, 3), own),
    )

    def d_body(sub, carry):
        tower_backward(sub, 32, d_in, d_up, *held, acc.at[D], pre_s, act_s, at_hooks(sub, steps))
        return carry

    tower_backward(0, 32, d_in, d_up, *held, acc.at[D], pre_s, act_s, at_hooks(0, steps), lambda step: d_loads[step].wait())
    lax.fori_loop(1, SUB_COUNT, d_body, 0)
    ex.pairs(D, ACROSS)
    ex.pairs(D, RIGHT)
    ex.rs_end(Q, OUTER)
    ex.start(Q, MIDDLE, FAR + NEAR)
    ex.settle(D, ACROSS)
    ex.pairs(D, LEFT)
    ex.rs_pass(Q, MIDDLE)
    ex.opened(Q, OUTER)
    ex.start(D, OUTER, FAR)
    ex.settle(D, RIGHT)
    ex.pairs(D, OWN)
    ex.rs_end(Q, MIDDLE)
    ex.start(Q, INNER, FAR + NEAR)
    ex.settle(D, LEFT, last=True)
    ex.start(D, OUTER, NEAR)
    ex.settle(D, OWN, last=True)
    ex.rs_pass(Q, INNER)
    ex.rs_pass(D, OUTER)
    ex.rs_end(Q, INNER)
    ex.opened(Q, INNER)
    ex.ag_start(Q, INNER)
    ex.rs_end(D, OUTER)
    ex.opened(Q, MIDDLE)
    ex.start(D, MIDDLE, FAR + NEAR)
    ex.ag_pass(Q, INNER)
    ex.ag_end(Q, INNER)
    ex.ag_start(Q, MIDDLE)
    ex.rs_pass(D, MIDDLE)
    ex.ag_pass(Q, MIDDLE)
    ex.rs_end(D, MIDDLE)
    ex.start(D, INNER, FAR + NEAR)
    ex.ag_end(Q, MIDDLE)
    ex.ag_start(Q, OUTER, FIRST)
    ex.rs_pass(D, INNER)
    ex.rs_end(D, INNER)
    ex.opened(D, INNER)
    ex.ag_start(D, INNER)
    ex.ag_start(Q, OUTER, SECOND)
    ex.ag_pass(D, INNER)
    ex.ag_pass(Q, OUTER)
    ex.ag_end(D, INNER)
    ex.opened(D, MIDDLE)
    ex.ag_start(D, MIDDLE)
    ex.ag_pass(D, MIDDLE)
    ex.ag_end(Q, OUTER)
    ex.ag_end(D, MIDDLE)
    ex.opened(D, OUTER)
    ex.ag_start(D, OUTER)
    ex.ag_pass(D, OUTER)
    ex.ag_end(D, OUTER)
    ex.finish()


def train(q_rows, d_rows, ups, weights):
    vmem, whole = pl.BlockSpec(memory_space=pltpu.VMEM), pl.BlockSpec(memory_space=pl.ANY)
    bufs = [pltpu.VMEM((3 * HALF // SIDE ** p // SIDE, 8, COLS), F32) for p in (OUTER, MIDDLE, INNER)]
    dma = pltpu.SemaphoreType.DMA
    return pl.pallas_call(
        train_kernel,
        out_shape=pltpu.VMEM((2, UNITS, 8, COLS), F32),
        in_specs=[whole] * 9,
        out_specs=vmem,
        scratch_shapes=[
            *[pltpu.VMEM(shape, BF16) for shape in WEIGHT_SHAPES],
            pltpu.VMEM((2, 32, FFN), F32),
            pltpu.VMEM((2, 32, FFN), BF16),
            pltpu.VMEM((2, 272, 8, COLS), F32),
            pltpu.VMEM(q_rows.shape, BF16),
            pltpu.VMEM(d_rows.shape, BF16),
            pltpu.VMEM(ups.shape, BF16),
            pltpu.SemaphoreType.DMA((3,)),
            *bufs,
            dma((5,)), *[dma((n,)) for n in (24, 24, 216, 216, 90, 90)],
            pltpu.SemaphoreType.REGULAR((2,)), pltpu.SemaphoreType.REGULAR((8,)),
        ],
        compiler_params=pltpu.CompilerParams(collective_id=1, has_side_effects=True, vmem_limit_bytes=TRAIN_VMEM),
        name='towers_backward_all_reduce',
    )(q_rows, d_rows, ups, *weights)


def unpack_kernel(acc, *rest):
    outs, sem = rest[:6], rest[6]
    copies = []
    for t in range(2):
        one, two, proj = outs[t * 3:t * 3 + 3]
        for k in range(2):
            for c in range(8):
                copies.append((acc.at[t, pl.ds(k * DIM + c * 64, 64)], one.at[k, :, :, pl.ds(c * COLS, COLS)]))
            for c in range(2):
                copies.append((acc.at[t, pl.ds(1024 + k * DIM + c * COLS, COLS)], two.at[k, :, :, pl.ds(c * COLS, COLS)]))
        for c in range(2):
            copies.append((acc.at[t, pl.ds(FFN + c * 64, 64)], proj.at[:, :, pl.ds(c * COLS, COLS)]))
    copies = [pltpu.make_async_copy(src, dst, sem.at[i]) for i, (src, dst) in enumerate(copies)]
    for c in copies:
        c.start()
    for c in copies:
        c.wait()


def unpack(acc):
    shapes = ((2, 64, 8, FFN), (2, COLS, 8, DIM), (64, 8, DIM)) * 2
    outs = pl.pallas_call(
        unpack_kernel,
        out_shape=tuple(jax.ShapeDtypeStruct(s, F32) for s in shapes),
        in_specs=[pl.BlockSpec(memory_space=pltpu.VMEM)],
        out_specs=(pl.BlockSpec(memory_space=pl.ANY),) * 6,
        scratch_shapes=[pltpu.SemaphoreType.DMA((44,))],
        compiler_params=pltpu.CompilerParams(vmem_limit_bytes=1 << 20),
        name='unpack',
    )(acc)
    return tuple(o.reshape(s) for o, s in zip(outs, WEIGHT_SHAPES * 2))


def local_step(q_loc, d_loc, temperature, *weights):
    d_rows = d_loc.reshape(-1, d_loc.shape[-1])
    ups, loss = scores(temperature.reshape(1), q_loc, d_rows, weights)
    return (loss.reshape(()), *unpack(train(q_loc, d_rows, ups, weights)))


def solution(mesh):
    specs_in = (P('data', None), P(None, 'data', None), P(), P(), P(), P(), P(), P(), P())
    specs_out = (P(), P(), P(), P(), P(), P(), P())
    return jax.shard_map(local_step, mesh=mesh, in_specs=specs_in, out_specs=specs_out, check_vma=False)
```
